512 devices in a mesh: groups: 2 (over y), prompt: 16 (over z), sample: 8 (over x), head: 2 (over core).
Axes of the slice: x: 8, y: 2, z: 16, core: 2. Of those that a mesh axis runs over, the one named last changes fastest.
The devices are a block of a 8x8x16 slice.
Arguments:
- queries: bfloat16 [1024, 16, 576], P(('groups', 'prompt', 'sample'), 'head'), parts along dimension 0, may hold values from -6 to 6
- prompt_cache: bfloat16 [64, 1024, 576], P(('groups', 'prompt'), 'sample'), parts along dimension 0, may hold values from -6 to 6
- suffix_cache: bfloat16 [1024, 64, 576], P(('groups', 'prompt', 'sample')), parts along dimension 0, may hold values from -6 to 6
- suffix_len: int32 [1024], P(('groups', 'prompt', 'sample')), parts along dimension 0, may hold values from 2 to 64, as said below
- sample_prompt: int32 [1024], P('groups'), parts along dimension 0, may hold values from 0 to 31, as said below
- prompt_slot: int32 [64], P('groups'), parts along dimension 0, may hold values from 0 to 31, as said below
Outputs:
- attended: bfloat16 [1024, 16, 512], P(('groups', 'prompt', 'sample'), 'head'), parts along dimension 0
The draws below stay inside these ranges and needn't reach their ends.
There are 2 independent parts, one for each index of `groups`. The reference program is written for one: setup_inputs(seed, part) draws one part's arguments, and reference() takes and returns one part's arrays. A program takes and returns all parts, laid end to end along the dimension named above; each array names one. Nothing has to cross between parts.
Inputs may be any that keep to these rules, and one draw needn't show every extreme that they name: `suffix_len`: the value 64 is reached. Every prompt is named by exactly 16 samples; in each aligned block of 4 samples, prompt_slot[sample_prompt] // 2 takes no value more than 1 times, and some value exactly 1 times. `prompt_slot`: a permutation.
All inputs are finite; a program needn't handle non-finite values.
Results may differ from the reference program's by a relative error of at most 0.013.
Values may be sent and summed in bfloat16 or wider, within the bound.
A program may use at most 64 MiB of HBM per device.

```python
import math
import jax
import jax.numpy as jnp
from jax import lax

H = 16
DL = 512
DR = 64
QKN = 128
SPP = 16
P_DEV = 2
PTOK = 1024
SUF = 64
PROMPTS = 32
S_DEV = 4
SAMPLES = 512


def base_field(key, shape):
    return jax.random.truncated_normal(key, -6.0, 6.0, shape, jnp.float32)


def keyed_field(key, salt, shape):
    field = base_field(jax.random.fold_in(key, salt), shape)
    return field.astype(jnp.bfloat16)


def draw_queries(key, part):
    field = base_field(jax.random.fold_in(key, 31), (SAMPLES, H, DL + DR))
    return field.astype(jnp.bfloat16)


def draw_prompt_cache(key, part):
    return keyed_field(key, 61, (PROMPTS, PTOK, DL + DR))


def draw_suffix_cache(key, part):
    return keyed_field(key, 71, (SAMPLES, SUF, DL + DR))


def draw_suffix_len(key, part):
    lengths = jax.random.randint(jax.random.fold_in(key, 51), (SAMPLES,), 2, SUF + 1)
    return lengths.at[0].set(SUF).astype(jnp.int32)


def routing_draw(key):
    owner_count = PROMPTS // P_DEV
    device_count = SAMPLES // S_DEV
    prompt_slot = jax.random.permutation(jax.random.fold_in(key, 41), PROMPTS)
    seats = jnp.repeat(jnp.arange(P_DEV, dtype=jnp.int32), SPP)
    owner_keys = jax.random.split(jax.random.fold_in(key, 42), owner_count)
    shuffled = jax.vmap(lambda single: jax.random.permutation(single, seats))(owner_keys)
    slots = (jnp.arange(owner_count, dtype=jnp.int32)[:, None] * P_DEV + shuffled).reshape(-1)
    dealt = slots.reshape(S_DEV, device_count).T
    device_order = jax.random.permutation(jax.random.fold_in(key, 44), device_count)
    per_device = dealt[jnp.argsort(device_order)]
    device_keys = jax.random.split(jax.random.fold_in(key, 43), device_count)
    orders = jax.vmap(lambda single: jax.random.permutation(single, S_DEV))(device_keys)
    per_device = jnp.take_along_axis(per_device, orders, axis=1)
    inverse = jnp.argsort(prompt_slot)
    sample_prompt = inverse[per_device.reshape(-1)]
    return (sample_prompt.astype(jnp.int32), prompt_slot.astype(jnp.int32))


def draw_sample_prompt(key, part):
    return routing_draw(key)[0]


def draw_prompt_slot(key, part):
    return routing_draw(key)[1]


def setup_inputs(seed: int = 0, part: int = 0) -> dict:
    seeds = jax.random.split(jax.random.key(seed), 7)
    own_keys = jax.random.split(jax.random.fold_in(seeds[6], part), 7)
    return {
        "queries": draw_queries(jax.random.fold_in(jax.random.fold_in(seeds[6], part), 71), part),
        "prompt_cache": draw_prompt_cache(jax.random.fold_in(jax.random.fold_in(seeds[6], part), 71), part),
        "suffix_cache": draw_suffix_cache(jax.random.fold_in(jax.random.fold_in(seeds[6], part), 71), part),
        "suffix_len": draw_suffix_len(jax.random.fold_in(jax.random.fold_in(seeds[6], part), 71), part),
        "sample_prompt": draw_sample_prompt(jax.random.fold_in(jax.random.fold_in(seeds[6], part), 71), part),
        "prompt_slot": draw_prompt_slot(jax.random.fold_in(jax.random.fold_in(seeds[6], part), 71), part),
    }


def reference(queries, prompt_cache, suffix_cache, suffix_len, sample_prompt, prompt_slot):
    scaling = 1.0 / math.sqrt(QKN + DR)
    members = jnp.argsort(sample_prompt, stable=True).astype(jnp.int32).reshape(PROMPTS, SPP)

    def per_prompt(prompt):
        chosen = members[prompt]
        asked = queries[chosen].astype(jnp.float32)
        shared = prompt_cache[prompt_slot[prompt]].astype(jnp.float32)
        recent = suffix_cache[chosen].astype(jnp.float32)
        lengths = suffix_len[chosen]
        shared_scores = jnp.einsum('shf,tf->sht', asked, shared) * scaling
        recent_scores = jnp.einsum('shf,stf->sht', asked, recent) * scaling
        allowed = jnp.arange(SUF, dtype=jnp.int32)[None, :] < lengths[:, None]
        recent_scores = jnp.where(allowed[:, None, :], recent_scores, -1e+30)
        row_max = jnp.maximum(lax.optimization_barrier(jnp.max(shared_scores, axis=-1)), lax.optimization_barrier(jnp.max(recent_scores, axis=-1)))
        shared_weights = jnp.exp(shared_scores - row_max[..., None])
        recent_weights = jnp.exp(recent_scores - row_max[..., None])
        row_sum = lax.optimization_barrier(jnp.sum(shared_weights, axis=-1)) + lax.optimization_barrier(jnp.sum(recent_weights, axis=-1))
        shared_rounded = lax.optimization_barrier(shared_weights.astype(jnp.bfloat16)).astype(jnp.float32)
        recent_rounded = lax.optimization_barrier(recent_weights.astype(jnp.bfloat16)).astype(jnp.float32)
        mixed = jnp.einsum('sht,td->shd', shared_rounded, shared[:, :DL])
        mixed = mixed + jnp.einsum('sht,std->shd', recent_rounded, recent[:, :, :DL])
        return (mixed / row_sum[..., None]).astype(jnp.bfloat16)
    results = lax.map(per_prompt, jnp.arange(PROMPTS, dtype=jnp.int32))
    output = jnp.zeros((SAMPLES, H, DL), jnp.bfloat16)
    return output.at[members.reshape(-1)].set(results.reshape(SAMPLES, H, DL))
```

```python
import functools
import math

import jax
import jax.numpy as jnp
from jax import lax
from jax.experimental import pallas as pl
from jax.experimental.pallas import tpu as pltpu
from jax.sharding import PartitionSpec as P

DL = 512
DR = 64
QKN = 128
P_DEV = 2
MESH = pl.DeviceIdType.MESH
NT = (((1,), (1,)), ((), ()))
F32 = jnp.float32
BF16 = jnp.bfloat16


def far_first(n):
    return sorted(range(1, n), key=lambda r: -min(r, n - r))


def kernel(
    n_own,
    n_slice,
    sp_ref,
    ps_ref,
    sl_ref,
    q_hbm,
    cache_hbm,
    suffix_hbm,
    out_ref,
    q_vm,
    keys,
    suf_vm,
    stage,
    arrived,
    asked,
    acc,
    top,
    tot,
    res,
    stat,
    ret,
    ret_stat,
    suf_out,
    suf_top,
    suf_tot,
    local_sem,
    ring_send,
    ring_recv,
    pair_send,
    pair_recv,
    q_send,
    q_recv,
    r_send,
    r_recv,
    s_send,
    s_recv,
):
    per_dev, heads, feat = q_vm.shape
    tok = cache_hbm.shape[2]
    half = feat // 2
    rows = n_own * heads
    scaling = 1.0 / math.sqrt(QKN + DR)
    z = lax.axis_index("prompt")
    x = lax.axis_index("sample")
    h = lax.axis_index("head")
    right = lax.rem(x + 1, n_slice)
    left = lax.rem(x + n_slice - 1, n_slice)
    partner = 1 - h

    load_q = pltpu.make_async_copy(q_hbm, q_vm, local_sem.at[0])
    load_cache = pltpu.make_async_copy(cache_hbm, keys.at[:, 0], local_sem.at[1])
    load_suffix = pltpu.make_async_copy(suffix_hbm, suf_vm, local_sem.at[2])
    load_q.start()
    load_cache.start()
    load_suffix.start()

    barrier = pltpu.get_barrier_semaphore()
    for r in far_first(n_own):
        pl.semaphore_signal(
            barrier, inc=1, device_id={"prompt": lax.rem(z + r, n_own)}, device_id_type=MESH
        )
    pl.semaphore_signal(barrier, inc=1, device_id={"sample": right}, device_id_type=MESH)
    pl.semaphore_signal(barrier, inc=1, device_id={"sample": left}, device_id_type=MESH)
    pl.semaphore_signal(barrier, inc=1, device_id={"head": partner}, device_id_type=MESH)

    own = (z * n_slice + x) * per_dev
    places = []
    for j in range(per_dev):
        slot = ps_ref[sp_ref[own + j]]
        places.append(lax.rem((slot >> 1) - z + n_own, n_own))

    load_q.wait()
    for r in range(n_own):
        pick = jnp.int32(0)
        for j in range(1, per_dev):
            pick = jnp.where(places[j] == r, j, pick)
        row = q_vm[pick]
        if r == 0:
            arrived[0] = row
        else:
            stage[r] = row

    row_place = lax.broadcasted_iota(jnp.int32, (rows, 128), 0) // heads
    parity = jnp.zeros((rows, 128), jnp.int32)
    for r in range(n_own):
        source = lax.rem(z - r + n_own, n_own)
        first = (source * n_slice + x) * per_dev
        odd = jnp.int32(0)
        for j in range(per_dev):
            slot = ps_ref[sp_ref[first + j]]
            odd = jnp.where((slot >> 1) == z, slot & 1, odd)
        parity = jnp.where(row_place == r, odd, parity)
    is_odd = parity[:, :1] > 0

    load_suffix.wait()
    suf_tokens = suf_vm.shape[1]
    token = lax.broadcasted_iota(jnp.int32, (heads, suf_tokens), 1)
    for j in range(per_dev):
        recent = suf_vm[j]
        s = lax.dot_general(q_vm[j], recent, NT, preferred_element_type=F32) * scaling
        s = jnp.where(token < sl_ref[j], s, -1e30)
        m = jnp.max(s, axis=1, keepdims=True)
        p = jnp.exp(s - m)
        suf_top[j] = jnp.broadcast_to(m, (heads, 128))
        suf_tot[j] = jnp.broadcast_to(jnp.sum(p, axis=1, keepdims=True), (heads, 128))
        suf_out[j] = jnp.dot(p.astype(BF16), recent[:, :DL], preferred_element_type=F32)

    load_cache.wait()
    pl.semaphore_wait(barrier, n_own - 1 + 3)

    last = n_slice // 2

    def slot_of(side, d):
        if d == 0:
            return 0
        if d == last:
            return n_slice - 1
        return 2 * d - 1 + side

    def part(side, d, piece):
        return keys.at[h, slot_of(side, d), pl.ds(piece * half, half), :]

    def pieces(side, d):
        order = (0, 1) if side == 0 else (1, 0)
        return order[:1] if d == last else order

    started = []

    def ring(side, d, piece):
        at = (side * last + d - 1) * 2 + piece
        return pltpu.make_async_remote_copy(
            src_ref=part(side, d - 1, piece),
            dst_ref=part(side, d, piece),
            send_sem=ring_send.at[at],
            recv_sem=ring_recv.at[at],
            device_id={"sample": right if side == 0 else left},
            device_id_type=MESH,
        )

    def pair(side, d, piece):
        at = (side * last + d - 1) * 2 + piece
        return pltpu.make_async_remote_copy(
            src_ref=part(side, d, piece),
            dst_ref=part(side, d, piece),
            send_sem=pair_send.at[at],
            recv_sem=pair_recv.at[at],
            device_id={"head": partner},
            device_id_type=MESH,
        )

    def pair_in(side, d, piece):
        at = (side * last + d - 1) * 2 + piece
        theirs = keys.at[partner, slot_of(side, d), pl.ds(piece * half, half), :]
        return pltpu.make_async_remote_copy(
            src_ref=theirs,
            dst_ref=theirs,
            send_sem=pair_send.at[at],
            recv_sem=pair_recv.at[at],
            device_id={"head": partner},
            device_id_type=MESH,
        )

    def start(copy):
        copy.start()
        started.append(copy)

    def start_ring(d):
        for k in range(len(pieces(0, d))):
            for side in (0, 1):
                start(ring(side, d, pieces(side, d)[k]))

    def service(d):
        for k in range(len(pieces(0, d))):
            for side in (0, 1):
                piece = pieces(side, d)[k]
                ring(side, d, piece).wait_recv()
                if d < last and piece in pieces(side, d + 1):
                    start(ring(side, d + 1, piece))
                start(pair(side, d, piece))

    def settle(d):
        for k in range(len(pieces(0, d))):
            for side in (0, 1):
                pair_in(side, d, pieces(side, d)[k]).wait_recv()

    def ask(r):
        return pltpu.make_async_remote_copy(
            src_ref=stage.at[r],
            dst_ref=arrived.at[r],
            send_sem=q_send.at[r],
            recv_sem=q_recv.at[r],
            device_id={"prompt": lax.rem(z + r, n_own)},
            device_id_type=MESH,
        )

    def answer(r):
        return pltpu.make_async_remote_copy(
            src_ref=res.at[r],
            dst_ref=ret.at[r],
            send_sem=r_send.at[r],
            recv_sem=r_recv.at[r],
            device_id={"prompt": lax.rem(z - r + n_own, n_own)},
            device_id_type=MESH,
        )

    def answer_stat(r):
        return pltpu.make_async_remote_copy(
            src_ref=stat.at[r],
            dst_ref=ret_stat.at[r],
            send_sem=s_send.at[r],
            recv_sem=s_recv.at[r],
            device_id={"prompt": lax.rem(z - r + n_own, n_own)},
            device_id_type=MESH,
        )

    start_ring(1)
    for r in far_first(n_own):
        start(ask(r))

    def attend(slots, first):
        q = asked[...]
        s0 = [jnp.dot(q, keys[0, k], preferred_element_type=F32) for k in slots]
        s1 = [jnp.dot(q, keys[1, k], preferred_element_type=F32) for k in slots]
        s = [jnp.where(is_odd, b, a) * scaling for a, b in zip(s0, s1)]
        m = functools.reduce(jnp.maximum, [jnp.max(a, axis=1, keepdims=True) for a in s])
        if not first:
            old = top[:, :1]
            m = jnp.maximum(m, old)
            fade = jnp.exp(old - m)
        p = [jnp.exp(a - m) for a in s]
        l = sum(jnp.sum(a, axis=1, keepdims=True) for a in p)
        out = 0.0
        for a, k in zip(p, slots):
            even = jnp.where(is_odd, 0.0, a).astype(BF16)
            odd = jnp.where(is_odd, a, 0.0).astype(BF16)
            out = out + lax.dot_general(even, keys[0, k, :DL], NT, preferred_element_type=F32)
            out = out + lax.dot_general(odd, keys[1, k, :DL], NT, preferred_element_type=F32)
        if not first:
            l = l + tot[:, :1] * fade
            out = out + acc[...] * fade
        top[...] = jnp.broadcast_to(m, (rows, 128))
        tot[...] = jnp.broadcast_to(l, (rows, 128))
        acc[...] = out

    def gather_asked():
        for r in far_first(n_own):
            ask(r).wait_recv()
        asked[...] = arrived[...].reshape(rows, feat)

    for d in range(1, last + 1):
        service(d)
        if d == max(1, last - 2):
            gather_asked()
            attend([0], True)
        if d < last and d >= max(1, last - 2):
            for e in range(1 if d == max(1, last - 2) else d, d + 1):
                settle(e)
                attend([2 * e - 1, 2 * e], False)
    settle(last)
    attend([n_slice - 1], False)

    m = top[...]
    l = tot[...]
    lane = lax.broadcasted_iota(jnp.int32, (rows, 128), 1)
    sub = lax.rem(lax.broadcasted_iota(jnp.int32, (rows, 128), 0), heads)
    both = jnp.where(lane == sub, m, 0.0) + jnp.where(lane == sub + heads, l, 0.0)
    both = jnp.sum(both.reshape(n_own, heads, 128), axis=1)
    for r in range(n_own):
        line = both[r : r + 1, :]
        block = acc[r * heads : (r + 1) * heads, :].astype(BF16)
        if r == 0:
            ret_stat[0] = line
            ret[0] = block
        else:
            stat[r] = line
            res[r] = block
    for r in far_first(n_own):
        start(answer(r))
        start(answer_stat(r))
    for r in far_first(n_own):
        answer(r).wait_recv()
        answer_stat(r).wait_recv()

    lane8 = lax.broadcasted_iota(jnp.int32, (heads, 128), 1)
    sub8 = lax.broadcasted_iota(jnp.int32, (heads, 128), 0)
    for j in range(per_dev):
        line = jnp.broadcast_to(ret_stat[places[j]], (heads, 128))
        pre_top = jnp.sum(jnp.where(lane8 == sub8, line, 0.0), axis=1, keepdims=True)
        pre_tot = jnp.sum(jnp.where(lane8 == sub8 + heads, line, 0.0), axis=1, keepdims=True)
        own_top = suf_top[j][:, :1]
        own_tot = suf_tot[j][:, :1]
        m = jnp.maximum(pre_top, own_top)
        w_pre = jnp.exp(pre_top - m)
        w_own = jnp.exp(own_top - m)
        total = w_pre * pre_tot + w_own * own_tot
        num = w_pre * ret[places[j]].astype(F32) + w_own * suf_out[j]
        out_ref[j] = (num / total).astype(out_ref.dtype)

    for copy in started:
        copy.wait_send()


def solution(mesh):
    n_own = mesh.shape["prompt"]
    n_slice = mesh.shape["sample"]

    def body(queries, prompt_cache, suffix_cache, suffix_len, sample_prompt, prompt_slot):
        per_dev, heads, feat = queries.shape
        tok = prompt_cache.shape[1]
        rows = n_own * heads
        ring = n_slice * 2
        dma = pltpu.SemaphoreType.DMA
        return pl.pallas_call(
            functools.partial(kernel, n_own, n_slice),
            out_shape=jax.ShapeDtypeStruct((per_dev, heads, DL), BF16),
            in_specs=[pl.BlockSpec(memory_space=pltpu.SMEM)] * 3
            + [pl.BlockSpec(memory_space=pl.ANY)] * 3,
            out_specs=pl.BlockSpec(memory_space=pltpu.VMEM),
            scratch_shapes=[
                pltpu.VMEM(queries.shape, BF16),
                pltpu.VMEM((P_DEV, n_slice, feat, tok), BF16),
                pltpu.VMEM(suffix_cache.shape, BF16),
                pltpu.VMEM((n_own, heads, feat), BF16),
                pltpu.VMEM((n_own, heads, feat), BF16),
                pltpu.VMEM((rows, feat), BF16),
                pltpu.VMEM((rows, DL), F32),
                pltpu.VMEM((rows, 128), F32),
                pltpu.VMEM((rows, 128), F32),
                pltpu.VMEM((n_own, heads, DL), BF16),
                pltpu.VMEM((n_own, 1, 128), F32),
                pltpu.VMEM((n_own, heads, DL), BF16),
                pltpu.VMEM((n_own, 1, 128), F32),
                pltpu.VMEM((per_dev, heads, DL), F32),
                pltpu.VMEM((per_dev, heads, 128), F32),
                pltpu.VMEM((per_dev, heads, 128), F32),
                dma((3,)),
                dma((ring,)),
                dma((ring,)),
                dma((ring,)),
                dma((ring,)),
                dma((n_own,)),
                dma((n_own,)),
                dma((n_own,)),
                dma((n_own,)),
                dma((n_own,)),
                dma((n_own,)),
            ],
            compiler_params=pltpu.CompilerParams(collective_id=0, has_side_effects=True),
        )(
            sample_prompt,
            prompt_slot,
            suffix_len,
            queries,
            jnp.swapaxes(prompt_cache, 1, 2),
            suffix_cache,
        )

    return jax.shard_map(
        body,
        mesh=mesh,
        in_specs=(
            P(("groups", "prompt", "sample"), "head", None),
            P(("groups", "prompt"), "sample", None),
            P(("groups", "prompt", "sample"), None, None),
            P(("groups", "prompt", "sample")),
            P("groups"),
            P("groups"),
        ),
        out_specs=P(("groups", "prompt", "sample"), "head", None),
        check_vma=False,
    )
```

```python
import functools
import math

import jax
import jax.numpy as jnp
from jax import lax
from jax.experimental import pallas as pl
from jax.experimental.pallas import tpu as pltpu
from jax.sharding import PartitionSpec as P

DL = 512
DR = 64
QKN = 128
P_DEV = 2
PIECES = 2
MESH = pl.DeviceIdType.MESH
NT = (((1,), (1,)), ((), ()))
F32 = jnp.float32
BF16 = jnp.bfloat16


def far_first(n):
    return sorted(range(1, n), key=lambda r: -min(r, n - r))


def kernel(
    n_own,
    n_slice,
    sp_hbm,
    ps_hbm,
    sl_hbm,
    q_hbm,
    cache_hbm,
    suffix_hbm,
    out_ref,
    sp_ref,
    ps_ref,
    sl_ref,
    q_vm,
    q_pair,
    keys,
    suf_vm,
    stage,
    arrived,
    asked,
    res,
    stat,
    ret,
    ret_stat,
    suf_out,
    suf_top,
    suf_tot,
    local_sem,
    ring_send,
    ring_recv,
    pair_send,
    pair_recv,
    raw_send,
    raw_recv,
    half_send,
    half_recv,
    q_send,
    q_recv,
    r_send,
    r_recv,
    s_send,
    s_recv,
):
    per_dev, heads, feat = q_vm.shape
    tok = cache_hbm.shape[2]
    rows = n_own * heads
    scaling = 1.0 / math.sqrt(QKN + DR)
    z = lax.axis_index("prompt")
    x = lax.axis_index("sample")
    h = lax.axis_index("head")
    right = lax.rem(x + 1, n_slice)
    left = lax.rem(x + n_slice - 1, n_slice)
    partner = 1 - h
    is_ring = h == 1
    is_post = h == 0

    loads = [
        pltpu.make_async_copy(cache_hbm, keys.at[:, :, pl.ds(0, tok)], local_sem.at[0]),
        pltpu.make_async_copy(q_hbm, q_vm, local_sem.at[1]),
        pltpu.make_async_copy(sp_hbm, sp_ref, local_sem.at[2]),
        pltpu.make_async_copy(ps_hbm, ps_ref, local_sem.at[3]),
        pltpu.make_async_copy(sl_hbm, sl_ref, local_sem.at[4]),
        pltpu.make_async_copy(suffix_hbm, suf_vm, local_sem.at[5]),
    ]
    for load in loads:
        load.start()

    barrier = pltpu.get_barrier_semaphore()
    pl.semaphore_signal(barrier, inc=1, device_id={"head": partner}, device_id_type=MESH)

    @pl.when(is_ring)
    def _():
        pl.semaphore_signal(barrier, inc=1, device_id={"sample": right}, device_id_type=MESH)
        pl.semaphore_signal(barrier, inc=1, device_id={"sample": left}, device_id_type=MESH)

    @pl.when(is_post)
    def _():
        for r in far_first(n_own):
            pl.semaphore_signal(
                barrier, inc=1, device_id={"prompt": lax.rem(z + r, n_own)}, device_id_type=MESH
            )

    last = n_slice // 2
    half = feat // PIECES

    def slot_of(side, d):
        if d == 0:
            return 0
        if d == last:
            return n_slice - 1
        return 2 * d - 1 + side

    def pieces(side, d):
        order = [side, 1 - side][: 1 if d == last else 2]
        return [(p, f) for p in order for f in range(PIECES)]

    def part(side, d, piece):
        p, f = piece
        return keys.at[p, pl.ds(f * half, half), pl.ds(slot_of(side, d) * tok, tok)]

    def sem_at(side, d, piece):
        p, f = piece
        return ((side * last + d - 1) * P_DEV + p) * PIECES + f

    def ring(side, d, piece):
        at = sem_at(side, d, piece)
        return pltpu.make_async_remote_copy(
            src_ref=part(side, d - 1, piece),
            dst_ref=part(side, d, piece),
            send_sem=ring_send.at[at],
            recv_sem=ring_recv.at[at],
            device_id={"sample": right if side == 0 else left},
            device_id_type=MESH,
        )

    def pair(side, d, piece):
        at = sem_at(side, d, piece)
        return pltpu.make_async_remote_copy(
            src_ref=part(side, d, piece),
            dst_ref=part(side, d, piece),
            send_sem=pair_send.at[at],
            recv_sem=pair_recv.at[at],
            device_id={"head": partner},
            device_id_type=MESH,
        )

    def every_piece():
        for d in range(1, last + 1):
            for k in range(len(pieces(0, d))):
                for side in (0, 1):
                    yield side, d, pieces(side, d)[k]

    def raw():
        return pltpu.make_async_remote_copy(
            src_ref=q_vm,
            dst_ref=q_pair,
            send_sem=raw_send.at[0],
            recv_sem=raw_recv.at[0],
            device_id={"head": partner},
            device_id_type=MESH,
        )

    def hand(r):
        return pltpu.make_async_remote_copy(
            src_ref=arrived.at[r, 1],
            dst_ref=arrived.at[r, 1],
            send_sem=half_send.at[r],
            recv_sem=half_recv.at[r],
            device_id={"head": partner},
            device_id_type=MESH,
        )

    def ask(r):
        return pltpu.make_async_remote_copy(
            src_ref=stage.at[r],
            dst_ref=arrived.at[r],
            send_sem=q_send.at[r],
            recv_sem=q_recv.at[r],
            device_id={"prompt": lax.rem(z + r, n_own)},
            device_id_type=MESH,
        )

    def answer(r):
        return pltpu.make_async_remote_copy(
            src_ref=res.at[r],
            dst_ref=ret.at[r],
            send_sem=r_send.at[r],
            recv_sem=r_recv.at[r],
            device_id={"prompt": lax.rem(z - r + n_own, n_own)},
            device_id_type=MESH,
        )

    def answer_stat(r):
        return pltpu.make_async_remote_copy(
            src_ref=stat.at[r],
            dst_ref=ret_stat.at[r],
            send_sem=s_send.at[r],
            recv_sem=s_recv.at[r],
            device_id={"prompt": lax.rem(z - r + n_own, n_own)},
            device_id_type=MESH,
        )

    own = (z * n_slice + x) * per_dev

    def own_places():
        return [
            lax.rem((ps_ref[sp_ref[own + j]] >> 1) - z + n_own, n_own) for j in range(per_dev)
        ]

    @pl.when(is_ring)
    def _():
        loads[1].wait()
        loads[0].wait()
        pl.semaphore_wait(barrier, 3)
        raw().start()
        for k in range(len(pieces(0, 1))):
            for side in (0, 1):
                ring(side, 1, pieces(side, 1)[k]).start()
        loads[2].wait()
        loads[3].wait()

    @pl.when(is_post)
    def _():
        loads[1].wait()
        loads[2].wait()
        loads[3].wait()
        picks = own_places()

        def row_of(r):
            pick = jnp.int32(0)
            for j in range(1, per_dev):
                pick = jnp.where(picks[j] == r, j, pick)
            return pick

        for r in far_first(n_own) + [0]:
            stage[r, 0] = q_vm[row_of(r)]
        pl.semaphore_wait(barrier, n_own)
        raw().wait_recv()
        for r in far_first(n_own) + [0]:
            stage[r, 1] = q_pair[row_of(r)]
        for r in far_first(n_own):
            ask(r).start()
        arrived[0] = stage[0]
        hand(0).start()
        loads[0].wait()

    loads[4].wait()
    loads[5].wait()
    suf_tokens = suf_vm.shape[1]
    token = lax.broadcasted_iota(jnp.int32, (heads, suf_tokens), 1)
    for j in range(per_dev):
        recent = suf_vm[j]
        s = lax.dot_general(q_vm[j], recent, NT, preferred_element_type=F32) * scaling
        s = jnp.where(token < sl_ref[j], s, -1e30)
        m = jnp.max(s, axis=1, keepdims=True)
        p = jnp.exp(s - m)
        suf_top[j] = jnp.broadcast_to(m, (heads, 128))
        suf_tot[j] = jnp.broadcast_to(jnp.sum(p, axis=1, keepdims=True), (heads, 128))
        suf_out[j] = jnp.dot(p.astype(BF16), recent[:, :DL], preferred_element_type=F32)

    row_place = lax.broadcasted_iota(jnp.int32, (rows, 128), 0) // heads
    parity = jnp.zeros((rows, 128), jnp.int32)
    for r in range(n_own):
        source = lax.rem(z - r + n_own, n_own)
        first = (source * n_slice + x) * per_dev
        odd = jnp.int32(0)
        for j in range(per_dev):
            slot = ps_ref[sp_ref[first + j]]
            odd = jnp.where((slot >> 1) == z, slot & 1, odd)
        parity = jnp.where(row_place == r, odd, parity)

    @pl.when(is_ring)
    def _():
        for side, d, piece in every_piece():
            ring(side, d, piece).wait_recv()
            if d < last and piece in pieces(side, d + 1):
                ring(side, d + 1, piece).start()
            pair(side, d, piece).start()
        for r in far_first(n_own)[::-1] + [0]:
            hand(r).wait_recv()
        asked[...] = arrived[:, 1].reshape(rows, feat)

    @pl.when(is_post)
    def _():
        for r in far_first(n_own)[::-1]:
            ask(r).wait_recv()
            hand(r).start()
        asked[...] = arrived[:, 0].reshape(rows, feat)
        for side, d, piece in every_piece():
            pair(side, d, piece).wait_recv()

    is_odd = parity[:, :1] > 0
    q = asked[...]
    s0 = jnp.dot(q, keys[0], preferred_element_type=F32)
    s1 = jnp.dot(q, keys[1], preferred_element_type=F32)
    s = jnp.where(is_odd, s1, s0) * scaling
    m = jnp.max(s, axis=1, keepdims=True)
    p = jnp.exp(s - m)
    l = jnp.sum(p, axis=1, keepdims=True)
    out = lax.dot_general(
        jnp.where(is_odd, 0.0, p).astype(BF16), keys[0, :DL], NT, preferred_element_type=F32
    ) + lax.dot_general(
        jnp.where(is_odd, p, 0.0).astype(BF16), keys[1, :DL], NT, preferred_element_type=F32
    )

    lane = lax.broadcasted_iota(jnp.int32, (rows, 128), 1)
    sub = lax.rem(lax.broadcasted_iota(jnp.int32, (rows, 128), 0), heads)
    both = jnp.where(lane == sub, m, 0.0) + jnp.where(lane == sub + heads, l, 0.0)
    both = jnp.sum(both.reshape(n_own, heads, 128), axis=1)
    for r in range(n_own):
        line = both[r : r + 1, :]
        block = out[r * heads : (r + 1) * heads, :].astype(BF16)
        if r == 0:
            ret_stat[0] = line
            ret[0] = block
        else:
            stat[r] = line
            res[r] = block
    for r in far_first(n_own):
        answer(r).start()
        answer_stat(r).start()

    places = own_places()
    for r in far_first(n_own)[::-1]:
        answer(r).wait_recv()
        answer_stat(r).wait_recv()

    lane8 = lax.broadcasted_iota(jnp.int32, (heads, 128), 1)
    sub8 = lax.broadcasted_iota(jnp.int32, (heads, 128), 0)
    for j in range(per_dev):
        line = jnp.broadcast_to(ret_stat[places[j]], (heads, 128))
        pre_top = jnp.sum(jnp.where(lane8 == sub8, line, 0.0), axis=1, keepdims=True)
        pre_tot = jnp.sum(jnp.where(lane8 == sub8 + heads, line, 0.0), axis=1, keepdims=True)
        own_top = suf_top[j][:, :1]
        own_tot = suf_tot[j][:, :1]
        m = jnp.maximum(pre_top, own_top)
        w_pre = jnp.exp(pre_top - m)
        w_own = jnp.exp(own_top - m)
        total = w_pre * pre_tot + w_own * own_tot
        num = w_pre * ret[places[j]].astype(F32) + w_own * suf_out[j]
        out_ref[j] = (num / total).astype(out_ref.dtype)

    for r in far_first(n_own):
        answer(r).wait_send()
        answer_stat(r).wait_send()

    @pl.when(is_ring)
    def _():
        raw().wait_send()
        for side, d, piece in every_piece():
            ring(side, d, piece).wait_send()
            pair(side, d, piece).wait_send()

    @pl.when(is_post)
    def _():
        for r in far_first(n_own):
            ask(r).wait_send()
        for r in range(n_own):
            hand(r).wait_send()


def solution(mesh):
    n_own = mesh.shape["prompt"]
    n_slice = mesh.shape["sample"]

    def body(queries, prompt_cache, suffix_cache, suffix_len, sample_prompt, prompt_slot):
        per_dev, heads, feat = queries.shape
        tok = prompt_cache.shape[1]
        rows = n_own * heads
        ring = n_slice * P_DEV * PIECES
        dma = pltpu.SemaphoreType.DMA
        return pl.pallas_call(
            functools.partial(kernel, n_own, n_slice),
            out_shape=jax.ShapeDtypeStruct((per_dev, heads, DL), BF16),
            in_specs=[pl.BlockSpec(memory_space=pl.ANY)] * 6,
            out_specs=pl.BlockSpec(memory_space=pltpu.VMEM),
            scratch_shapes=[
                pltpu.SMEM(sample_prompt.shape, jnp.int32),
                pltpu.SMEM(prompt_slot.shape, jnp.int32),
                pltpu.SMEM(suffix_len.shape, jnp.int32),
                pltpu.VMEM(queries.shape, BF16),
                pltpu.VMEM(queries.shape, BF16),
                pltpu.VMEM((P_DEV, feat, n_slice * tok), BF16),
                pltpu.VMEM(suffix_cache.shape, BF16),
                pltpu.VMEM((n_own, 2, heads, feat), BF16),
                pltpu.VMEM((n_own, 2, heads, feat), BF16),
                pltpu.VMEM((rows, feat), BF16),
                pltpu.VMEM((n_own, heads, DL), BF16),
                pltpu.VMEM((n_own, 1, 128), F32),
                pltpu.VMEM((n_own, heads, DL), BF16),
                pltpu.VMEM((n_own, 1, 128), F32),
                pltpu.VMEM((per_dev, heads, DL), F32),
                pltpu.VMEM((per_dev, heads, 128), F32),
                pltpu.VMEM((per_dev, heads, 128), F32),
                dma((6,)),
                dma((ring,)),
                dma((ring,)),
                dma((ring,)),
                dma((ring,)),
                dma((1,)),
                dma((1,)),
                dma((n_own,)),
                dma((n_own,)),
                dma((n_own,)),
                dma((n_own,)),
                dma((n_own,)),
                dma((n_own,)),
                dma((n_own,)),
                dma((n_own,)),
            ],
            compiler_params=pltpu.CompilerParams(collective_id=0, has_side_effects=True),
        )(
            sample_prompt,
            prompt_slot,
            suffix_len,
            queries,
            jnp.swapaxes(prompt_cache, 1, 2),
            suffix_cache,
        )

    return jax.shard_map(
        body,
        mesh=mesh,
        in_specs=(
            P(("groups", "prompt", "sample"), "head", None),
            P(("groups", "prompt"), "sample", None),
            P(("groups", "prompt", "sample"), None, None),
            P(("groups", "prompt", "sample")),
            P("groups"),
            P("groups"),
        ),
        out_specs=P(("groups", "prompt", "sample"), "head", None),
        check_vma=False,
    )
```

```python
import functools
import math

import jax
import jax.numpy as jnp
from jax import lax
from jax.experimental import pallas as pl
from jax.experimental.pallas import tpu as pltpu
from jax.sharding import PartitionSpec as P

DL = 512
DR = 64
QKN = 128
P_DEV = 2
POST = 0
PIECES = 2
MESH = pl.DeviceIdType.MESH
NT = (((1,), (1,)), ((), ()))
F32 = jnp.float32
BF16 = jnp.bfloat16


def far_first(n):
    return sorted(range(1, n), key=lambda r: -min(r, n - r))


def kernel(
    n_own,
    n_slice,
    sp_hbm,
    ps_hbm,
    sl_hbm,
    q_hbm,
    cache_hbm,
    suffix_hbm,
    out_ref,
    sp_ref,
    ps_ref,
    sl_ref,
    q_vm,
    q_pair,
    keys,
    suf_vm,
    stage,
    arrived,
    res,
    stat,
    ret,
    ret_stat,
    suf_out,
    suf_top,
    suf_tot,
    local_sem,
    ring_send,
    ring_recv,
    pair_send,
    pair_recv,
    raw_send,
    raw_recv,
    q_send,
    q_recv,
    r_send,
    r_recv,
    s_send,
    s_recv,
):
    per_dev, heads, feat = q_vm.shape
    tok = cache_hbm.shape[2]
    rows = n_own * heads
    scaling = 1.0 / math.sqrt(QKN + DR)
    z = lax.axis_index("prompt")
    x = lax.axis_index("sample")
    h = lax.axis_index("head")
    right = lax.rem(x + 1, n_slice)
    left = lax.rem(x + n_slice - 1, n_slice)
    partner = 1 - h
    is_ring = h != POST
    is_post = h == POST

    loads = [
        pltpu.make_async_copy(cache_hbm, keys.at[:, :, pl.ds(0, tok)], local_sem.at[0]),
        pltpu.make_async_copy(q_hbm, q_vm, local_sem.at[1]),
        pltpu.make_async_copy(sp_hbm, sp_ref, local_sem.at[2]),
        pltpu.make_async_copy(ps_hbm, ps_ref, local_sem.at[3]),
        pltpu.make_async_copy(sl_hbm, sl_ref, local_sem.at[4]),
        pltpu.make_async_copy(suffix_hbm, suf_vm, local_sem.at[5]),
    ]
    for load in loads:
        load.start()

    barrier = pltpu.get_barrier_semaphore()
    pl.semaphore_signal(barrier, inc=1, device_id={"head": partner}, device_id_type=MESH)

    @pl.when(is_ring)
    def _():
        pl.semaphore_signal(barrier, inc=1, device_id={"sample": right}, device_id_type=MESH)
        pl.semaphore_signal(barrier, inc=1, device_id={"sample": left}, device_id_type=MESH)
        for r in far_first(n_own):
            pl.semaphore_signal(
                barrier,
                inc=1,
                device_id={"prompt": lax.rem(z + r, n_own), "head": POST},
                device_id_type=MESH,
            )

    @pl.when(is_post)
    def _():
        for r in far_first(n_own):
            pl.semaphore_signal(
                barrier, inc=1, device_id={"prompt": lax.rem(z + r, n_own)}, device_id_type=MESH
            )

    last = n_slice // 2
    half = feat // PIECES

    def slot_of(side, d):
        if d == 0:
            return 0
        if d == last:
            return n_slice - 1
        return 2 * d - 1 + side

    def pieces(side, d):
        order = [side, 1 - side][: 1 if d == last else 2]
        return [(p, f) for p in order for f in range(PIECES)]

    def part(side, d, piece):
        p, f = piece
        return keys.at[p, pl.ds(f * half, half), pl.ds(slot_of(side, d) * tok, tok)]

    def sem_at(side, d, piece):
        p, f = piece
        return ((side * last + d - 1) * P_DEV + p) * PIECES + f

    def ring(side, d, piece):
        at = sem_at(side, d, piece)
        return pltpu.make_async_remote_copy(
            src_ref=part(side, d - 1, piece),
            dst_ref=part(side, d, piece),
            send_sem=ring_send.at[at],
            recv_sem=ring_recv.at[at],
            device_id={"sample": right if side == 0 else left},
            device_id_type=MESH,
        )

    def pair(side, d, piece):
        at = sem_at(side, d, piece)
        return pltpu.make_async_remote_copy(
            src_ref=part(side, d, piece),
            dst_ref=part(side, d, piece),
            send_sem=pair_send.at[at],
            recv_sem=pair_recv.at[at],
            device_id={"head": partner},
            device_id_type=MESH,
        )

    def every_piece():
        for d in range(1, last + 1):
            for k in range(len(pieces(0, d))):
                for side in (0, 1):
                    yield side, d, pieces(side, d)[k]

    def raw():
        return pltpu.make_async_remote_copy(
            src_ref=q_vm,
            dst_ref=q_pair,
            send_sem=raw_send.at[0],
            recv_sem=raw_recv.at[0],
            device_id={"head": partner},
            device_id_type=MESH,
        )

    def hand():
        return pltpu.make_async_remote_copy(
            src_ref=stage.at[1, 0],
            dst_ref=arrived.at[0],
            send_sem=q_send.at[1, 0],
            recv_sem=q_recv.at[0],
            device_id={"head": partner},
            device_id_type=MESH,
        )

    def ask(side, r):
        return pltpu.make_async_remote_copy(
            src_ref=stage.at[side, r],
            dst_ref=arrived.at[r],
            send_sem=q_send.at[side, r],
            recv_sem=q_recv.at[r],
            device_id={
                "prompt": lax.rem(z + r, n_own),
                "head": POST if side == 0 else 1 - POST,
            },
            device_id_type=MESH,
        )

    def answer(r):
        return pltpu.make_async_remote_copy(
            src_ref=res.at[r],
            dst_ref=ret.at[r],
            send_sem=r_send.at[r],
            recv_sem=r_recv.at[r],
            device_id={"prompt": lax.rem(z - r + n_own, n_own)},
            device_id_type=MESH,
        )

    def answer_stat(r):
        return pltpu.make_async_remote_copy(
            src_ref=stat.at[r],
            dst_ref=ret_stat.at[r],
            send_sem=s_send.at[r],
            recv_sem=s_recv.at[r],
            device_id={"prompt": lax.rem(z - r + n_own, n_own)},
            device_id_type=MESH,
        )

    own = (z * n_slice + x) * per_dev

    def own_places():
        return [
            lax.rem((ps_ref[sp_ref[own + j]] >> 1) - z + n_own, n_own) for j in range(per_dev)
        ]

    @pl.when(is_ring)
    def _():
        loads[1].wait()
        loads[0].wait()
        pl.semaphore_wait(barrier, 3)
        raw().start()
        for k in range(len(pieces(0, 1))):
            for side in (0, 1):
                ring(side, 1, pieces(side, 1)[k]).start()
        loads[2].wait()
        loads[3].wait()

    @pl.when(is_post)
    def _():
        loads[1].wait()
        loads[2].wait()
        loads[3].wait()
        picks = own_places()

        def row_of(r):
            pick = jnp.int32(0)
            for j in range(1, per_dev):
                pick = jnp.where(picks[j] == r, j, pick)
            return pick

        for r in far_first(n_own) + [0]:
            stage[0, r] = q_vm[row_of(r)]
        arrived[0] = stage[0, 0]
        pl.semaphore_wait(barrier, 2 * n_own - 1)
        for r in far_first(n_own):
            ask(0, r).start()
        raw().wait_recv()
        for r in far_first(n_own) + [0]:
            stage[1, r] = q_pair[row_of(r)]
        for r in far_first(n_own):
            ask(1, r).start()
        hand().start()
        loads[0].wait()

    loads[4].wait()
    loads[5].wait()
    suf_tokens = suf_vm.shape[1]
    token = lax.broadcasted_iota(jnp.int32, (heads, suf_tokens), 1)
    for j in range(per_dev):
        recent = suf_vm[j]
        s = lax.dot_general(q_vm[j], recent, NT, preferred_element_type=F32) * scaling
        s = jnp.where(token < sl_ref[j], s, -1e30)
        m = jnp.max(s, axis=1, keepdims=True)
        p = jnp.exp(s - m)
        suf_top[j] = jnp.broadcast_to(m, (heads, 128))
        suf_tot[j] = jnp.broadcast_to(jnp.sum(p, axis=1, keepdims=True), (heads, 128))
        suf_out[j] = jnp.dot(p.astype(BF16), recent[:, :DL], preferred_element_type=F32)

    row_place = lax.broadcasted_iota(jnp.int32, (rows, 128), 0) // heads
    parity = jnp.zeros((rows, 128), jnp.int32)
    for r in range(n_own):
        source = lax.rem(z - r + n_own, n_own)
        first = (source * n_slice + x) * per_dev
        odd = jnp.int32(0)
        for j in range(per_dev):
            slot = ps_ref[sp_ref[first + j]]
            odd = jnp.where((slot >> 1) == z, slot & 1, odd)
        parity = jnp.where(row_place == r, odd, parity)

    @pl.when(is_ring)
    def _():
        for side, d, piece in every_piece():
            ring(side, d, piece).wait_recv()
            if d < last and piece in pieces(side, d + 1):
                ring(side, d + 1, piece).start()
            pair(side, d, piece).start()
        hand().wait_recv()

    @pl.when(is_post)
    def _():
        for side, d, piece in every_piece():
            pair(side, d, piece).wait_recv()

    for r in far_first(n_own)[::-1]:
        ask(0, r).wait_recv()

    is_odd = parity[:, :1] > 0
    q = arrived[...].reshape(rows, feat)
    s0 = jnp.dot(q, keys[0], preferred_element_type=F32)
    s1 = jnp.dot(q, keys[1], preferred_element_type=F32)
    s = jnp.where(is_odd, s1, s0) * scaling
    m = jnp.max(s, axis=1, keepdims=True)
    p = jnp.exp(s - m)
    l = jnp.sum(p, axis=1, keepdims=True)
    out = lax.dot_general(
        jnp.where(is_odd, 0.0, p).astype(BF16), keys[0, :DL], NT, preferred_element_type=F32
    ) + lax.dot_general(
        jnp.where(is_odd, p, 0.0).astype(BF16), keys[1, :DL], NT, preferred_element_type=F32
    )

    lane = lax.broadcasted_iota(jnp.int32, (rows, 128), 1)
    sub = lax.rem(lax.broadcasted_iota(jnp.int32, (rows, 128), 0), heads)
    both = jnp.where(lane == sub, m, 0.0) + jnp.where(lane == sub + heads, l, 0.0)
    both = jnp.sum(both.reshape(n_own, heads, 128), axis=1)
    for r in range(n_own):
        line = both[r : r + 1, :]
        block = out[r * heads : (r + 1) * heads, :].astype(BF16)
        if r == 0:
            ret_stat[0] = line
            ret[0] = block
        else:
            stat[r] = line
            res[r] = block
    for r in far_first(n_own):
        answer(r).start()
        answer_stat(r).start()

    places = own_places()
    for r in far_first(n_own)[::-1]:
        answer(r).wait_recv()
        answer_stat(r).wait_recv()

    lane8 = lax.broadcasted_iota(jnp.int32, (heads, 128), 1)
    sub8 = lax.broadcasted_iota(jnp.int32, (heads, 128), 0)
    for j in range(per_dev):
        line = jnp.broadcast_to(ret_stat[places[j]], (heads, 128))
        pre_top = jnp.sum(jnp.where(lane8 == sub8, line, 0.0), axis=1, keepdims=True)
        pre_tot = jnp.sum(jnp.where(lane8 == sub8 + heads, line, 0.0), axis=1, keepdims=True)
        own_top = suf_top[j][:, :1]
        own_tot = suf_tot[j][:, :1]
        m = jnp.maximum(pre_top, own_top)
        w_pre = jnp.exp(pre_top - m)
        w_own = jnp.exp(own_top - m)
        total = w_pre * pre_tot + w_own * own_tot
        num = w_pre * ret[places[j]].astype(F32) + w_own * suf_out[j]
        out_ref[j] = (num / total).astype(out_ref.dtype)

    for r in far_first(n_own):
        answer(r).wait_send()
        answer_stat(r).wait_send()

    @pl.when(is_ring)
    def _():
        raw().wait_send()
        for side, d, piece in every_piece():
            ring(side, d, piece).wait_send()
            pair(side, d, piece).wait_send()

    @pl.when(is_post)
    def _():
        for r in far_first(n_own):
            ask(0, r).wait_send()
            ask(1, r).wait_send()
        hand().wait_send()


def solution(mesh):
    n_own = mesh.shape["prompt"]
    n_slice = mesh.shape["sample"]

    def body(queries, prompt_cache, suffix_cache, suffix_len, sample_prompt, prompt_slot):
        per_dev, heads, feat = queries.shape
        tok = prompt_cache.shape[1]
        ring = n_slice * P_DEV * PIECES
        dma = pltpu.SemaphoreType.DMA
        return pl.pallas_call(
            functools.partial(kernel, n_own, n_slice),
            out_shape=jax.ShapeDtypeStruct((per_dev, heads, DL), BF16),
            in_specs=[pl.BlockSpec(memory_space=pltpu.HBM)] * 6,
            out_specs=pl.BlockSpec(memory_space=pltpu.VMEM),
            scratch_shapes=[
                pltpu.SMEM(sample_prompt.shape, jnp.int32),
                pltpu.SMEM(prompt_slot.shape, jnp.int32),
                pltpu.SMEM(suffix_len.shape, jnp.int32),
                pltpu.VMEM(queries.shape, BF16),
                pltpu.VMEM(queries.shape, BF16),
                pltpu.VMEM((P_DEV, feat, n_slice * tok), BF16),
                pltpu.VMEM(suffix_cache.shape, BF16),
                pltpu.VMEM((2, n_own, heads, feat), BF16),
                pltpu.VMEM((n_own, heads, feat), BF16),
                pltpu.VMEM((n_own, heads, DL), BF16),
                pltpu.VMEM((n_own, 1, 128), F32),
                pltpu.VMEM((n_own, heads, DL), BF16),
                pltpu.VMEM((n_own, 1, 128), F32),
                pltpu.VMEM((per_dev, heads, DL), F32),
                pltpu.VMEM((per_dev, heads, 128), F32),
                pltpu.VMEM((per_dev, heads, 128), F32),
                dma((6,)),
                dma((ring,)),
                dma((ring,)),
                dma((ring,)),
                dma((ring,)),
                dma((1,)),
                dma((1,)),
                dma((2, n_own)),
                dma((n_own,)),
                dma((n_own,)),
                dma((n_own,)),
                dma((n_own,)),
                dma((n_own,)),
            ],
            compiler_params=pltpu.CompilerParams(collective_id=0, has_side_effects=True),
        )(
            sample_prompt,
            prompt_slot,
            suffix_len,
            queries,
            jnp.swapaxes(prompt_cache, 1, 2),
            suffix_cache,
        )

    return jax.shard_map(
        body,
        mesh=mesh,
        in_specs=(
            P(("groups", "prompt", "sample"), "head", None),
            P(("groups", "prompt"), "sample", None),
            P(("groups", "prompt", "sample"), None, None),
            P(("groups", "prompt", "sample")),
            P("groups"),
            P("groups"),
        ),
        out_specs=P(("groups", "prompt", "sample"), "head", None),
        check_vma=False,
    )
```

```python
import functools
import math

import jax
import jax.numpy as jnp
from jax import lax
from jax.experimental import pallas as pl
from jax.experimental.pallas import tpu as pltpu
from jax.sharding import PartitionSpec as P

DL = 512
DR = 64
QKN = 128
P_DEV = 2
POST = 0
PIECES = 2
SHARE = 8
MESH = pl.DeviceIdType.MESH
NT = (((1,), (1,)), ((), ()))
F32 = jnp.float32
BF16 = jnp.bfloat16


def far_first(n):
    return sorted(range(1, n), key=lambda r: -min(r, n - r))


def kernel(
    n_own,
    n_slice,
    sp_hbm,
    ps_hbm,
    sl_hbm,
    q_hbm,
    cache_hbm,
    suffix_hbm,
    out_ref,
    sp_ref,
    ps_ref,
    sl_ref,
    q_vm,
    q_pair,
    keys,
    suf_vm,
    stage,
    arrived,
    res,
    stat,
    ret,
    ret_stat,
    suf_out,
    suf_top,
    suf_tot,
    parity,
    local_sem,
    ring_send,
    ring_recv,
    pair_send,
    pair_recv,
    raw_send,
    raw_recv,
    q_send,
    q_recv,
    r_send,
    r_recv,
    s_send,
    s_recv,
):
    per_dev, heads, feat = q_vm.shape
    tok = cache_hbm.shape[2]
    rows = n_own * heads
    scaling = 1.0 / math.sqrt(QKN + DR)
    z = lax.axis_index("prompt")
    x = lax.axis_index("sample")
    h = lax.axis_index("head")
    right = lax.rem(x + 1, n_slice)
    left = lax.rem(x + n_slice - 1, n_slice)
    partner = 1 - h
    is_ring = h != POST
    is_post = h == POST

    loads = [
        pltpu.make_async_copy(cache_hbm, keys.at[:, :, pl.ds(0, tok)], local_sem.at[0]),
        pltpu.make_async_copy(q_hbm, q_vm, local_sem.at[1]),
        pltpu.make_async_copy(sp_hbm, sp_ref, local_sem.at[2]),
        pltpu.make_async_copy(ps_hbm, ps_ref, local_sem.at[3]),
        pltpu.make_async_copy(sl_hbm, sl_ref, local_sem.at[4]),
        pltpu.make_async_copy(suffix_hbm, suf_vm, local_sem.at[5]),
    ]
    for load in loads:
        load.start()

    barrier = pltpu.get_barrier_semaphore()
    pl.semaphore_signal(barrier, inc=1, device_id={"head": partner}, device_id_type=MESH)

    @pl.when(is_ring)
    def _():
        pl.semaphore_signal(barrier, inc=1, device_id={"sample": right}, device_id_type=MESH)
        pl.semaphore_signal(barrier, inc=1, device_id={"sample": left}, device_id_type=MESH)
        for r in far_first(n_own):
            pl.semaphore_signal(
                barrier,
                inc=1,
                device_id={"prompt": lax.rem(z + r, n_own), "head": POST},
                device_id_type=MESH,
            )

    @pl.when(is_post)
    def _():
        for r in far_first(n_own):
            pl.semaphore_signal(
                barrier, inc=1, device_id={"prompt": lax.rem(z + r, n_own)}, device_id_type=MESH
            )

    last = n_slice // 2
    half = feat // PIECES

    def slot_of(side, d):
        if d == 0:
            return 0
        if d == last:
            return n_slice - 1
        return 2 * d - 1 + side

    def pieces(side, d):
        order = [side, 1 - side][: 1 if d == last else 2]
        return [(p, f) for p in order for f in range(PIECES)]

    def part(side, d, piece):
        p, f = piece
        return keys.at[p, pl.ds(f * half, half), pl.ds(slot_of(side, d) * tok, tok)]

    def sem_at(side, d, piece):
        p, f = piece
        return ((side * last + d - 1) * P_DEV + p) * PIECES + f

    def ring(side, d, piece):
        at = sem_at(side, d, piece)
        return pltpu.make_async_remote_copy(
            src_ref=part(side, d - 1, piece),
            dst_ref=part(side, d, piece),
            send_sem=ring_send.at[at],
            recv_sem=ring_recv.at[at],
            device_id={"sample": right if side == 0 else left},
            device_id_type=MESH,
        )

    def pair(side, d, piece):
        at = sem_at(side, d, piece)
        return pltpu.make_async_remote_copy(
            src_ref=part(side, d, piece),
            dst_ref=part(side, d, piece),
            send_sem=pair_send.at[at],
            recv_sem=pair_recv.at[at],
            device_id={"head": partner},
            device_id_type=MESH,
        )

    def every_piece():
        for d in range(1, last + 1):
            for k in range(len(pieces(0, d))):
                for side in (0, 1):
                    yield side, d, pieces(side, d)[k]

    def raw():
        return pltpu.make_async_remote_copy(
            src_ref=q_vm,
            dst_ref=q_pair,
            send_sem=raw_send.at[0],
            recv_sem=raw_recv.at[0],
            device_id={"head": partner},
            device_id_type=MESH,
        )

    def hand():
        return pltpu.make_async_remote_copy(
            src_ref=stage.at[1, z],
            dst_ref=arrived.at[z],
            send_sem=q_send.at[1, z],
            recv_sem=q_recv.at[z],
            device_id={"head": partner},
            device_id_type=MESH,
        )

    def ask(side, row):
        return pltpu.make_async_remote_copy(
            src_ref=stage.at[side, row],
            dst_ref=arrived.at[z],
            send_sem=q_send.at[side, row],
            recv_sem=q_recv.at[z],
            device_id={"prompt": row, "head": POST if side == 0 else 1 - POST},
            device_id_type=MESH,
        )

    def asked_by(row):
        return pltpu.make_async_remote_copy(
            src_ref=stage.at[0, row],
            dst_ref=arrived.at[row],
            send_sem=q_send.at[0, row],
            recv_sem=q_recv.at[row],
            device_id={"prompt": row},
            device_id_type=MESH,
        )

    def answer(row):
        return pltpu.make_async_remote_copy(
            src_ref=res.at[row],
            dst_ref=ret.at[z],
            send_sem=r_send.at[row],
            recv_sem=r_recv.at[z],
            device_id={"prompt": row},
            device_id_type=MESH,
        )

    def answer_stat(row):
        return pltpu.make_async_remote_copy(
            src_ref=stat.at[row],
            dst_ref=ret_stat.at[z],
            send_sem=s_send.at[row],
            recv_sem=s_recv.at[z],
            device_id={"prompt": row},
            device_id_type=MESH,
        )

    def answered_by(row):
        return [
            pltpu.make_async_remote_copy(
                src_ref=source.at[row],
                dst_ref=target.at[row],
                send_sem=send.at[row],
                recv_sem=recv.at[row],
                device_id={"prompt": row},
                device_id_type=MESH,
            )
            for source, target, send, recv in (
                (res, ret, r_send, r_recv),
                (stat, ret_stat, s_send, s_recv),
            )
        ]

    own = (z * n_slice + x) * per_dev

    def own_places():
        return [ps_ref[sp_ref[own + j]] >> 1 for j in range(per_dev)]

    def others():
        return [lax.rem(z + r, n_own) for r in far_first(n_own)]

    def recent_part():
        loads[4].wait()
        loads[5].wait()
        suf_tokens = suf_vm.shape[1]
        token = lax.broadcasted_iota(jnp.int32, (heads, suf_tokens), 1)
        for j in range(per_dev):
            recent = suf_vm[j]
            s = lax.dot_general(q_vm[j], recent, NT, preferred_element_type=F32) * scaling
            s = jnp.where(token < sl_ref[j], s, -1e30)
            m = jnp.max(s, axis=1, keepdims=True)
            p = jnp.exp(s - m)
            suf_top[j] = jnp.broadcast_to(m, (heads, 128))
            suf_tot[j] = jnp.broadcast_to(jnp.sum(p, axis=1, keepdims=True), (heads, 128))
            suf_out[j] = jnp.dot(p.astype(BF16), recent[:, :DL], preferred_element_type=F32)

        row_place = lax.broadcasted_iota(jnp.int32, (rows, 128), 0) // heads
        odds = jnp.zeros((rows, 128), jnp.int32)
        for row in range(n_own):
            first = (row * n_slice + x) * per_dev
            odd = jnp.int32(0)
            for j in range(per_dev):
                slot = ps_ref[sp_ref[first + j]]
                odd = jnp.where((slot >> 1) == z, slot & 1, odd)
            odds = jnp.where(row_place == row, odd, odds)
        parity[...] = odds

    @pl.when(is_ring)
    def _():
        loads[1].wait()
        loads[0].wait()
        pl.semaphore_wait(barrier, 3)
        raw().start()
        for k in range(len(pieces(0, 1))):
            for side in (0, 1):
                ring(side, 1, pieces(side, 1)[k]).start()
        loads[2].wait()
        loads[3].wait()
        recent_part()
        for side, d, piece in every_piece():
            ring(side, d, piece).wait_recv()
            if d < last and piece in pieces(side, d + 1):
                ring(side, d + 1, piece).start()
            pair(side, d, piece).start()

    @pl.when(is_post)
    def _():
        for load in loads[:4]:
            load.wait()
        picks = own_places()

        def sample_of(row):
            pick = jnp.int32(0)
            for j in range(1, per_dev):
                pick = jnp.where(picks[j] == row, j, pick)
            return pick

        for row in range(n_own):
            stage[0, row] = q_vm[sample_of(row)]
        recent_part()
        raw().wait_recv()
        for row in range(n_own):
            stage[1, row] = q_pair[sample_of(row)]
        arrived[z] = stage[0, z]
        pl.semaphore_wait(barrier, 2 * n_own - 1)
        for row in others():
            ask(0, row).start()
            ask(1, row).start()
        hand().start()
        for side, d, piece in every_piece():
            pair(side, d, piece).wait_recv()

    def attend(lo, hi):
        for row in range(lo, hi):

            @pl.when(jnp.logical_or(is_ring, z != row))
            def _():
                asked_by(row).wait_recv()

        size = (hi - lo) * heads
        is_odd = parity[lo * heads : hi * heads, :1] > 0
        q = arrived[lo:hi].reshape(size, feat)
        s0 = jnp.dot(q, keys[0], preferred_element_type=F32)
        s1 = jnp.dot(q, keys[1], preferred_element_type=F32)
        s = jnp.where(is_odd, s1, s0) * scaling
        m = jnp.max(s, axis=1, keepdims=True)
        p = jnp.exp(s - m)
        l = jnp.sum(p, axis=1, keepdims=True)
        out = lax.dot_general(
            jnp.where(is_odd, 0.0, p).astype(BF16), keys[0, :DL], NT, preferred_element_type=F32
        ) + lax.dot_general(
            jnp.where(is_odd, p, 0.0).astype(BF16), keys[1, :DL], NT, preferred_element_type=F32
        )
        lane = lax.broadcasted_iota(jnp.int32, (size, 128), 1)
        sub = lax.rem(lax.broadcasted_iota(jnp.int32, (size, 128), 0), heads)
        both = jnp.where(lane == sub, m, 0.0) + jnp.where(lane == sub + heads, l, 0.0)
        both = jnp.sum(both.reshape(hi - lo, heads, 128), axis=1)
        for row in range(lo, hi):
            at = row - lo
            stat[row] = both[at : at + 1, :]
            res[row] = out[at * heads : (at + 1) * heads, :].astype(BF16)
        for row in range(lo, hi):

            @pl.when(z != row)
            def _():
                answer(row).start()
                answer_stat(row).start()

    cuts = [0, n_own // SHARE, n_own]
    for lo, hi in zip(cuts, cuts[1:]):
        attend(lo, hi)
    ret[z] = res[z]
    ret_stat[z] = stat[z]

    places = own_places()
    for row in range(n_own):

        @pl.when(z != row)
        def _():
            for copy in answered_by(row):
                copy.wait_recv()

    lane8 = lax.broadcasted_iota(jnp.int32, (heads, 128), 1)
    sub8 = lax.broadcasted_iota(jnp.int32, (heads, 128), 0)
    for j in range(per_dev):
        line = jnp.broadcast_to(ret_stat[places[j]], (heads, 128))
        pre_top = jnp.sum(jnp.where(lane8 == sub8, line, 0.0), axis=1, keepdims=True)
        pre_tot = jnp.sum(jnp.where(lane8 == sub8 + heads, line, 0.0), axis=1, keepdims=True)
        own_top = suf_top[j][:, :1]
        own_tot = suf_tot[j][:, :1]
        m = jnp.maximum(pre_top, own_top)
        w_pre = jnp.exp(pre_top - m)
        w_own = jnp.exp(own_top - m)
        total = w_pre * pre_tot + w_own * own_tot
        num = w_pre * ret[places[j]].astype(F32) + w_own * suf_out[j]
        out_ref[j] = (num / total).astype(out_ref.dtype)

    for row in others():
        answer(row).wait_send()
        answer_stat(row).wait_send()

    @pl.when(is_ring)
    def _():
        raw().wait_send()
        for side, d, piece in every_piece():
            ring(side, d, piece).wait_send()
            pair(side, d, piece).wait_send()

    @pl.when(is_post)
    def _():
        for row in others():
            ask(0, row).wait_send()
            ask(1, row).wait_send()
        hand().wait_send()


def solution(mesh):
    n_own = mesh.shape["prompt"]
    n_slice = mesh.shape["sample"]

    def body(queries, prompt_cache, suffix_cache, suffix_len, sample_prompt, prompt_slot):
        per_dev, heads, feat = queries.shape
        tok = prompt_cache.shape[1]
        ring = n_slice * P_DEV * PIECES
        dma = pltpu.SemaphoreType.DMA
        return pl.pallas_call(
            functools.partial(kernel, n_own, n_slice),
            out_shape=jax.ShapeDtypeStruct((per_dev, heads, DL), BF16),
            in_specs=[pl.BlockSpec(memory_space=pltpu.HBM)] * 6,
            out_specs=pl.BlockSpec(memory_space=pltpu.VMEM),
            scratch_shapes=[
                pltpu.SMEM(sample_prompt.shape, jnp.int32),
                pltpu.SMEM(prompt_slot.shape, jnp.int32),
                pltpu.SMEM(suffix_len.shape, jnp.int32),
                pltpu.VMEM(queries.shape, BF16),
                pltpu.VMEM(queries.shape, BF16),
                pltpu.VMEM((P_DEV, feat, n_slice * tok), BF16),
                pltpu.VMEM(suffix_cache.shape, BF16),
                pltpu.VMEM((2, n_own, heads, feat), BF16),
                pltpu.VMEM((n_own, heads, feat), BF16),
                pltpu.VMEM((n_own, heads, DL), BF16),
                pltpu.VMEM((n_own, 1, 128), F32),
                pltpu.VMEM((n_own, heads, DL), BF16),
                pltpu.VMEM((n_own, 1, 128), F32),
                pltpu.VMEM((per_dev, heads, DL), F32),
                pltpu.VMEM((per_dev, heads, 128), F32),
                pltpu.VMEM((per_dev, heads, 128), F32),
                pltpu.VMEM((n_own * heads, 128), jnp.int32),
                dma((6,)),
                dma((ring,)),
                dma((ring,)),
                dma((ring,)),
                dma((ring,)),
                dma((1,)),
                dma((1,)),
                dma((2, n_own)),
                dma((n_own,)),
                dma((n_own,)),
                dma((n_own,)),
                dma((n_own,)),
                dma((n_own,)),
            ],
            compiler_params=pltpu.CompilerParams(collective_id=0, has_side_effects=True),
        )(
            sample_prompt,
            prompt_slot,
            suffix_len,
            queries,
            jnp.swapaxes(prompt_cache, 1, 2),
            suffix_cache,
        )

    return jax.shard_map(
        body,
        mesh=mesh,
        in_specs=(
            P(("groups", "prompt", "sample"), "head", None),
            P(("groups", "prompt"), "sample", None),
            P(("groups", "prompt", "sample"), None, None),
            P(("groups", "prompt", "sample")),
            P("groups"),
            P("groups"),
        ),
        out_specs=P(("groups", "prompt", "sample"), "head", None),
        check_vma=False,
    )
```

```python
import functools
import math

import jax
import jax.numpy as jnp
from jax import lax
from jax.experimental import pallas as pl
from jax.experimental.pallas import tpu as pltpu
from jax.sharding import PartitionSpec as P

DL = 512
DR = 64
QKN = 128
P_DEV = 2
POST = 0
PIECES = 2
SHARE = 8
MESH = pl.DeviceIdType.MESH
NT = (((1,), (1,)), ((), ()))
F32 = jnp.float32
BF16 = jnp.bfloat16


def far_first(n):
    return sorted(range(1, n), key=lambda r: -min(r, n - r))


def kernel(
    n_own,
    n_slice,
    sp_hbm,
    ps_hbm,
    sl_hbm,
    q_hbm,
    cache_hbm,
    suffix_hbm,
    out_ref,
    sp_ref,
    ps_ref,
    sl_ref,
    q_vm,
    q_pair,
    keys,
    suf_vm,
    stage,
    arrived,
    res,
    stat,
    ret,
    ret_stat,
    suf_out,
    suf_top,
    suf_tot,
    parity,
    part_top,
    part_tot,
    part_out,
    local_sem,
    ring_send,
    ring_recv,
    pair_send,
    pair_recv,
    raw_send,
    raw_recv,
    q_send,
    q_recv,
    r_send,
    r_recv,
    s_send,
    s_recv,
):
    per_dev, heads, feat = q_vm.shape
    tok = cache_hbm.shape[2]
    rows = n_own * heads
    scaling = 1.0 / math.sqrt(QKN + DR)
    z = lax.axis_index("prompt")
    x = lax.axis_index("sample")
    h = lax.axis_index("head")
    right = lax.rem(x + 1, n_slice)
    left = lax.rem(x + n_slice - 1, n_slice)
    partner = 1 - h
    is_ring = h != POST
    is_post = h == POST

    loads = [
        pltpu.make_async_copy(cache_hbm, keys.at[:, :, pl.ds(0, tok)], local_sem.at[0]),
        pltpu.make_async_copy(q_hbm, q_vm, local_sem.at[1]),
        pltpu.make_async_copy(sp_hbm, sp_ref, local_sem.at[2]),
        pltpu.make_async_copy(ps_hbm, ps_ref, local_sem.at[3]),
        pltpu.make_async_copy(sl_hbm, sl_ref, local_sem.at[4]),
        pltpu.make_async_copy(suffix_hbm, suf_vm, local_sem.at[5]),
    ]
    for load in loads[:5]:
        load.start()

    barrier = pltpu.get_barrier_semaphore()
    pl.semaphore_signal(barrier, inc=1, device_id={"head": partner}, device_id_type=MESH)

    @pl.when(is_ring)
    def _():
        pl.semaphore_signal(barrier, inc=1, device_id={"sample": right}, device_id_type=MESH)
        pl.semaphore_signal(barrier, inc=1, device_id={"sample": left}, device_id_type=MESH)
        for r in far_first(n_own):
            pl.semaphore_signal(
                barrier,
                inc=1,
                device_id={"prompt": lax.rem(z + r, n_own), "head": POST},
                device_id_type=MESH,
            )

    @pl.when(is_post)
    def _():
        for r in far_first(n_own):
            pl.semaphore_signal(
                barrier, inc=1, device_id={"prompt": lax.rem(z + r, n_own)}, device_id_type=MESH
            )

    last = n_slice // 2
    half = feat // PIECES

    def slot_of(side, d):
        if d == 0:
            return 0
        if d == last:
            return n_slice - 1
        return 2 * d - 1 + side

    def pieces(side, d):
        order = [side, 1 - side][: 1 if d == last else 2]
        return [(p, f) for p in order for f in range(PIECES)]

    def part(side, d, piece):
        p, f = piece
        return keys.at[p, pl.ds(f * half, half), pl.ds(slot_of(side, d) * tok, tok)]

    def sem_at(side, d, piece):
        p, f = piece
        return ((side * last + d - 1) * P_DEV + p) * PIECES + f

    def ring(side, d, piece):
        at = sem_at(side, d, piece)
        return pltpu.make_async_remote_copy(
            src_ref=part(side, d - 1, piece),
            dst_ref=part(side, d, piece),
            send_sem=ring_send.at[at],
            recv_sem=ring_recv.at[at],
            device_id={"sample": right if side == 0 else left},
            device_id_type=MESH,
        )

    def pair(side, d, piece):
        at = sem_at(side, d, piece)
        return pltpu.make_async_remote_copy(
            src_ref=part(side, d, piece),
            dst_ref=part(side, d, piece),
            send_sem=pair_send.at[at],
            recv_sem=pair_recv.at[at],
            device_id={"head": partner},
            device_id_type=MESH,
        )

    def every_piece():
        for d in range(1, last + 1):
            for k in range(len(pieces(0, d))):
                for side in (0, 1):
                    yield side, d, pieces(side, d)[k]

    def raw():
        return pltpu.make_async_remote_copy(
            src_ref=q_vm,
            dst_ref=q_pair,
            send_sem=raw_send.at[0],
            recv_sem=raw_recv.at[0],
            device_id={"head": partner},
            device_id_type=MESH,
        )

    def hand():
        return pltpu.make_async_remote_copy(
            src_ref=stage.at[1, z],
            dst_ref=arrived.at[z],
            send_sem=q_send.at[1, z],
            recv_sem=q_recv.at[z],
            device_id={"head": partner},
            device_id_type=MESH,
        )

    def ask(side, row):
        return pltpu.make_async_remote_copy(
            src_ref=stage.at[side, row],
            dst_ref=arrived.at[z],
            send_sem=q_send.at[side, row],
            recv_sem=q_recv.at[z],
            device_id={"prompt": row, "head": POST if side == 0 else 1 - POST},
            device_id_type=MESH,
        )

    def asked_by(row):
        return pltpu.make_async_remote_copy(
            src_ref=stage.at[0, row],
            dst_ref=arrived.at[row],
            send_sem=q_send.at[0, row],
            recv_sem=q_recv.at[row],
            device_id={"prompt": row},
            device_id_type=MESH,
        )

    def answer(row):
        return pltpu.make_async_remote_copy(
            src_ref=res.at[row],
            dst_ref=ret.at[z],
            send_sem=r_send.at[row],
            recv_sem=r_recv.at[z],
            device_id={"prompt": row},
            device_id_type=MESH,
        )

    def answer_stat(row):
        return pltpu.make_async_remote_copy(
            src_ref=stat.at[row],
            dst_ref=ret_stat.at[z],
            send_sem=s_send.at[row],
            recv_sem=s_recv.at[z],
            device_id={"prompt": row},
            device_id_type=MESH,
        )

    def answered_by(row):
        return [
            pltpu.make_async_remote_copy(
                src_ref=source.at[row],
                dst_ref=target.at[row],
                send_sem=send.at[row],
                recv_sem=recv.at[row],
                device_id={"prompt": row},
                device_id_type=MESH,
            )
            for source, target, send, recv in (
                (res, ret, r_send, r_recv),
                (stat, ret_stat, s_send, s_recv),
            )
        ]

    own = (z * n_slice + x) * per_dev

    def own_places():
        return [ps_ref[sp_ref[own + j]] >> 1 for j in range(per_dev)]

    def others():
        return [lax.rem(z + r, n_own) for r in far_first(n_own)]

    def recent_part(j):
        recent = suf_vm[j]
        token = lax.broadcasted_iota(jnp.int32, (heads, recent.shape[0]), 1)
        s = lax.dot_general(q_vm[j], recent, NT, preferred_element_type=F32) * scaling
        s = jnp.where(token < sl_ref[j], s, -1e30)
        m = jnp.max(s, axis=1, keepdims=True)
        p = jnp.exp(s - m)
        suf_top[j] = jnp.broadcast_to(m, (heads, 128))
        suf_tot[j] = jnp.broadcast_to(jnp.sum(p, axis=1, keepdims=True), (heads, 128))
        suf_out[j] = jnp.dot(p.astype(BF16), recent[:, :DL], preferred_element_type=F32)

    def parity_part():
        place = lax.broadcasted_iota(jnp.int32, (heads, 128), 0)
        for row in range(n_own):
            first = (row * n_slice + x) * per_dev
            odd = jnp.int32(0)
            for j in range(per_dev):
                slot = ps_ref[sp_ref[first + j]]
                odd = jnp.where((slot >> 1) == z, slot & 1, odd)
            parity[row * heads : (row + 1) * heads, :] = jnp.where(place >= 0, odd, 0)

    @pl.when(is_ring)
    def _():
        loads[0].wait()
        pl.semaphore_wait(barrier, 3)
        for k in range(len(pieces(0, 1))):
            for side in (0, 1):
                ring(side, 1, pieces(side, 1)[k]).start()
        loads[5].start()
        loads[1].wait()
        raw().start()
        for load in loads[2:]:
            load.wait()
        filler = [functools.partial(recent_part, j) for j in range(per_dev)] + [parity_part]
        for k, (side, d, piece) in enumerate(every_piece()):
            ring(side, d, piece).wait_recv()
            if d < last and piece in pieces(side, d + 1):
                ring(side, d + 1, piece).start()
            pair(side, d, piece).start()
            if k % 2 == 1 and filler:
                filler.pop(0)()

    @pl.when(is_post)
    def _():
        for load in loads[:4]:
            load.wait()
        picks = own_places()

        def sample_of(row):
            pick = jnp.int32(0)
            for j in range(1, per_dev):
                pick = jnp.where(picks[j] == row, j, pick)
            return pick

        for row in range(n_own):
            stage[0, row] = q_vm[sample_of(row)]
        loads[5].start()
        raw().wait_recv()
        for row in range(n_own):
            stage[1, row] = q_pair[sample_of(row)]
        arrived[z] = stage[0, z]
        pl.semaphore_wait(barrier, 2 * n_own - 1)
        for row in others():
            ask(0, row).start()
            ask(1, row).start()
        hand().start()
        loads[4].wait()
        loads[5].wait()
        parity_part()
        for j in range(per_dev):
            recent_part(j)
        for side, d, piece in every_piece():
            if d < last:
                pair(side, d, piece).wait_recv()

    def collect(lo, hi):
        for row in range(lo, hi):

            @pl.when(jnp.logical_or(is_ring, z != row))
            def _():
                asked_by(row).wait_recv()

    def weigh(lo, hi, begin, end):
        size = (hi - lo) * heads
        is_odd = parity[lo * heads : hi * heads, :1] > 0
        q = arrived[lo:hi].reshape(size, feat)
        s0 = jnp.dot(q, keys[0, :, begin:end], preferred_element_type=F32)
        s1 = jnp.dot(q, keys[1, :, begin:end], preferred_element_type=F32)
        s = jnp.where(is_odd, s1, s0) * scaling
        m = jnp.max(s, axis=1, keepdims=True)
        p = jnp.exp(s - m)
        l = jnp.sum(p, axis=1, keepdims=True)
        even = jnp.where(is_odd, 0.0, p).astype(BF16)
        odd = jnp.where(is_odd, p, 0.0).astype(BF16)
        out = lax.dot_general(
            even, keys[0, :DL, begin:end], NT, preferred_element_type=F32
        ) + lax.dot_general(odd, keys[1, :DL, begin:end], NT, preferred_element_type=F32)
        return m, l, out

    def give(lo, hi, m, l, out):
        size = (hi - lo) * heads
        lane = lax.broadcasted_iota(jnp.int32, (size, 128), 1)
        sub = lax.rem(lax.broadcasted_iota(jnp.int32, (size, 128), 0), heads)
        both = jnp.where(lane == sub, m, 0.0) + jnp.where(lane == sub + heads, l, 0.0)
        both = jnp.sum(both.reshape(hi - lo, heads, 128), axis=1)
        for row in range(lo, hi):
            at = row - lo
            stat[row] = both[at : at + 1, :]
            res[row] = out[at * heads : (at + 1) * heads, :].astype(BF16)
        for row in range(lo, hi):

            @pl.when(z != row)
            def _():
                answer(row).start()
                answer_stat(row).start()

    cut = n_own // SHARE
    near = (n_slice - 1) * tok
    collect(0, cut)
    m0, l0, out0 = weigh(0, cut, 0, near)
    part_top[...] = jnp.broadcast_to(m0, (cut * heads, 128))
    part_tot[...] = jnp.broadcast_to(l0, (cut * heads, 128))
    part_out[...] = out0

    @pl.when(is_post)
    def _():
        for side, d, piece in every_piece():
            if d == last:
                pair(side, d, piece).wait_recv()

    m1, l1, out1 = weigh(0, cut, near, near + tok)
    m0 = part_top[:, :1]
    m = jnp.maximum(m0, m1)
    fade0 = jnp.exp(m0 - m)
    fade1 = jnp.exp(m1 - m)
    give(0, cut, m, part_tot[:, :1] * fade0 + l1 * fade1, part_out[...] * fade0 + out1 * fade1)
    collect(cut, n_own)
    give(cut, n_own, *weigh(cut, n_own, 0, n_slice * tok))
    ret[z] = res[z]
    ret_stat[z] = stat[z]

    for row in others():
        answer(row).wait_send()
        answer_stat(row).wait_send()

    @pl.when(is_ring)
    def _():
        raw().wait_send()
        for side, d, piece in every_piece():
            ring(side, d, piece).wait_send()
            pair(side, d, piece).wait_send()

    @pl.when(is_post)
    def _():
        for row in others():
            ask(0, row).wait_send()
            ask(1, row).wait_send()
        hand().wait_send()

    places = own_places()
    for row in range(n_own):

        @pl.when(z != row)
        def _():
            for copy in answered_by(row):
                copy.wait_recv()

    lane8 = lax.broadcasted_iota(jnp.int32, (heads, 128), 1)
    sub8 = lax.broadcasted_iota(jnp.int32, (heads, 128), 0)
    for j in range(per_dev):
        line = jnp.broadcast_to(ret_stat[places[j]], (heads, 128))
        pre_top = jnp.sum(jnp.where(lane8 == sub8, line, 0.0), axis=1, keepdims=True)
        pre_tot = jnp.sum(jnp.where(lane8 == sub8 + heads, line, 0.0), axis=1, keepdims=True)
        own_top = suf_top[j][:, :1]
        own_tot = suf_tot[j][:, :1]
        m = jnp.maximum(pre_top, own_top)
        w_pre = jnp.exp(pre_top - m)
        w_own = jnp.exp(own_top - m)
        total = w_pre * pre_tot + w_own * own_tot
        num = w_pre * ret[places[j]].astype(F32) + w_own * suf_out[j]
        out_ref[j] = (num / total).astype(out_ref.dtype)


def solution(mesh):
    n_own = mesh.shape["prompt"]
    n_slice = mesh.shape["sample"]

    def body(queries, prompt_cache, suffix_cache, suffix_len, sample_prompt, prompt_slot):
        per_dev, heads, feat = queries.shape
        tok = prompt_cache.shape[1]
        ring = n_slice * P_DEV * PIECES
        dma = pltpu.SemaphoreType.DMA
        return pl.pallas_call(
            functools.partial(kernel, n_own, n_slice),
            out_shape=jax.ShapeDtypeStruct((per_dev, heads, DL), BF16),
            in_specs=[pl.BlockSpec(memory_space=pltpu.HBM)] * 6,
            out_specs=pl.BlockSpec(memory_space=pltpu.VMEM),
            scratch_shapes=[
                pltpu.SMEM(sample_prompt.shape, jnp.int32),
                pltpu.SMEM(prompt_slot.shape, jnp.int32),
                pltpu.SMEM(suffix_len.shape, jnp.int32),
                pltpu.VMEM(queries.shape, BF16),
                pltpu.VMEM(queries.shape, BF16),
                pltpu.VMEM((P_DEV, feat, n_slice * tok), BF16),
                pltpu.VMEM(suffix_cache.shape, BF16),
                pltpu.VMEM((2, n_own, heads, feat), BF16),
                pltpu.VMEM((n_own, heads, feat), BF16),
                pltpu.VMEM((n_own, heads, DL), BF16),
                pltpu.VMEM((n_own, 1, 128), F32),
                pltpu.VMEM((n_own, heads, DL), BF16),
                pltpu.VMEM((n_own, 1, 128), F32),
                pltpu.VMEM((per_dev, heads, DL), F32),
                pltpu.VMEM((per_dev, heads, 128), F32),
                pltpu.VMEM((per_dev, heads, 128), F32),
                pltpu.VMEM((n_own * heads, 128), jnp.int32),
                pltpu.VMEM((n_own // SHARE * heads, 128), F32),
                pltpu.VMEM((n_own // SHARE * heads, 128), F32),
                pltpu.VMEM((n_own // SHARE * heads, DL), F32),
                dma((6,)),
                dma((ring,)),
                dma((ring,)),
                dma((ring,)),
                dma((ring,)),
                dma((1,)),
                dma((1,)),
                dma((2, n_own)),
                dma((n_own,)),
                dma((n_own,)),
                dma((n_own,)),
                dma((n_own,)),
                dma((n_own,)),
            ],
            compiler_params=pltpu.CompilerParams(collective_id=0, has_side_effects=True),
        )(
            sample_prompt,
            prompt_slot,
            suffix_len,
            queries,
            jnp.swapaxes(prompt_cache, 1, 2),
            suffix_cache,
        )

    return jax.shard_map(
        body,
        mesh=mesh,
        in_specs=(
            P(("groups", "prompt", "sample"), "head", None),
            P(("groups", "prompt"), "sample", None),
            P(("groups", "prompt", "sample"), None, None),
            P(("groups", "prompt", "sample")),
            P("groups"),
            P("groups"),
        ),
        out_specs=P(("groups", "prompt", "sample"), "head", None),
        check_vma=False,
    )
```

```python
import functools
import math

import jax
import jax.numpy as jnp
from jax import lax
from jax.experimental import pallas as pl
from jax.experimental.pallas import tpu as pltpu
from jax.sharding import PartitionSpec as P

DL = 512
DR = 64
QKN = 128
P_DEV = 2
POST = 0
PIECES = 2
SHARE = 8
MESH = pl.DeviceIdType.MESH
NT = (((1,), (1,)), ((), ()))
F32 = jnp.float32
BF16 = jnp.bfloat16


def far_first(n):
    return sorted(range(1, n), key=lambda r: -min(r, n - r))


def kernel(
    n_own,
    n_slice,
    sp_hbm,
    ps_hbm,
    sl_hbm,
    q_hbm,
    cache_hbm,
    suffix_hbm,
    out_ref,
    sp_ref,
    ps_ref,
    sl_ref,
    q_vm,
    q_pair,
    keys,
    suf_vm,
    stage,
    arrived,
    res,
    stat,
    ret,
    ret_stat,
    suf_out,
    suf_top,
    suf_tot,
    parity,
    part_top,
    part_tot,
    part_out,
    local_sem,
    ring_send,
    ring_recv,
    pair_send,
    pair_recv,
    raw_send,
    raw_recv,
    q_send,
    q_recv,
    r_send,
    r_recv,
    s_send,
    s_recv,
):
    per_dev, heads, feat = q_vm.shape
    tok = cache_hbm.shape[2]
    rows = n_own * heads
    scaling = 1.0 / math.sqrt(QKN + DR)
    z = lax.axis_index("prompt")
    x = lax.axis_index("sample")
    h = lax.axis_index("head")
    right = lax.rem(x + 1, n_slice)
    left = lax.rem(x + n_slice - 1, n_slice)
    partner = 1 - h
    is_ring = h != POST
    is_post = h == POST

    loads = [
        pltpu.make_async_copy(cache_hbm, keys.at[:, :, pl.ds(0, tok)], local_sem.at[0]),
        pltpu.make_async_copy(q_hbm, q_vm, local_sem.at[1]),
        pltpu.make_async_copy(sp_hbm, sp_ref, local_sem.at[2]),
        pltpu.make_async_copy(ps_hbm, ps_ref, local_sem.at[3]),
        pltpu.make_async_copy(sl_hbm, sl_ref, local_sem.at[4]),
        pltpu.make_async_copy(suffix_hbm, suf_vm, local_sem.at[5]),
    ]
    for load in loads:
        load.start()

    barrier = pltpu.get_barrier_semaphore()
    pl.semaphore_signal(barrier, inc=1, device_id={"head": partner}, device_id_type=MESH)

    @pl.when(is_ring)
    def _():
        pl.semaphore_signal(barrier, inc=1, device_id={"sample": right}, device_id_type=MESH)
        pl.semaphore_signal(barrier, inc=1, device_id={"sample": left}, device_id_type=MESH)
        for r in far_first(n_own):
            pl.semaphore_signal(
                barrier,
                inc=1,
                device_id={"prompt": lax.rem(z + r, n_own), "head": POST},
                device_id_type=MESH,
            )

    @pl.when(is_post)
    def _():
        for r in far_first(n_own):
            pl.semaphore_signal(
                barrier, inc=1, device_id={"prompt": lax.rem(z + r, n_own)}, device_id_type=MESH
            )

    last = n_slice // 2
    half = feat // PIECES

    def slot_of(side, d):
        if d == 0:
            return 0
        if d == last:
            return n_slice - 1
        return 2 * d - 1 + side

    def pieces(side, d):
        order = [side, 1 - side][: 1 if d == last else 2]
        return [(p, f) for p in order for f in range(PIECES)]

    def part(side, d, piece):
        p, f = piece
        return keys.at[p, pl.ds(f * half, half), pl.ds(slot_of(side, d) * tok, tok)]

    def sem_at(side, d, piece):
        p, f = piece
        return ((side * last + d - 1) * P_DEV + p) * PIECES + f

    def ring(side, d, piece):
        at = sem_at(side, d, piece)
        return pltpu.make_async_remote_copy(
            src_ref=part(side, d - 1, piece),
            dst_ref=part(side, d, piece),
            send_sem=ring_send.at[at],
            recv_sem=ring_recv.at[at],
            device_id={"sample": right if side == 0 else left},
            device_id_type=MESH,
        )

    def pair(side, d, piece):
        at = sem_at(side, d, piece)
        return pltpu.make_async_remote_copy(
            src_ref=part(side, d, piece),
            dst_ref=part(side, d, piece),
            send_sem=pair_send.at[at],
            recv_sem=pair_recv.at[at],
            device_id={"head": partner},
            device_id_type=MESH,
        )

    def every_piece():
        for d in range(1, last + 1):
            for k in range(len(pieces(0, d))):
                for side in (0, 1):
                    yield side, d, pieces(side, d)[k]

    def raw():
        return pltpu.make_async_remote_copy(
            src_ref=q_vm,
            dst_ref=q_pair,
            send_sem=raw_send.at[0],
            recv_sem=raw_recv.at[0],
            device_id={"head": partner},
            device_id_type=MESH,
        )

    def hand():
        return pltpu.make_async_remote_copy(
            src_ref=stage.at[1, z],
            dst_ref=arrived.at[z],
            send_sem=q_send.at[1, z],
            recv_sem=q_recv.at[z],
            device_id={"head": partner},
            device_id_type=MESH,
        )

    def ask(side, row):
        return pltpu.make_async_remote_copy(
            src_ref=stage.at[side, row],
            dst_ref=arrived.at[z],
            send_sem=q_send.at[side, row],
            recv_sem=q_recv.at[z],
            device_id={"prompt": row, "head": POST if side == 0 else 1 - POST},
            device_id_type=MESH,
        )

    def asked_by(row):
        return pltpu.make_async_remote_copy(
            src_ref=stage.at[0, row],
            dst_ref=arrived.at[row],
            send_sem=q_send.at[0, row],
            recv_sem=q_recv.at[row],
            device_id={"prompt": row},
            device_id_type=MESH,
        )

    def answer(row):
        return pltpu.make_async_remote_copy(
            src_ref=res.at[row],
            dst_ref=ret.at[z],
            send_sem=r_send.at[row],
            recv_sem=r_recv.at[z],
            device_id={"prompt": row},
            device_id_type=MESH,
        )

    def answer_stat(row):
        return pltpu.make_async_remote_copy(
            src_ref=stat.at[row],
            dst_ref=ret_stat.at[z],
            send_sem=s_send.at[row],
            recv_sem=s_recv.at[z],
            device_id={"prompt": row},
            device_id_type=MESH,
        )

    def answered_by(row):
        return [
            pltpu.make_async_remote_copy(
                src_ref=source.at[row],
                dst_ref=target.at[row],
                send_sem=send.at[row],
                recv_sem=recv.at[row],
                device_id={"prompt": row},
                device_id_type=MESH,
            )
            for source, target, send, recv in (
                (res, ret, r_send, r_recv),
                (stat, ret_stat, s_send, s_recv),
            )
        ]

    own = (z * n_slice + x) * per_dev

    def own_places():
        return [ps_ref[sp_ref[own + j]] >> 1 for j in range(per_dev)]

    def others():
        return [lax.rem(z + r, n_own) for r in far_first(n_own)]

    def recent_part(j):
        recent = suf_vm[j]
        token = lax.broadcasted_iota(jnp.int32, (heads, recent.shape[0]), 1)
        s = lax.dot_general(q_vm[j], recent, NT, preferred_element_type=F32) * scaling
        s = jnp.where(token < sl_ref[j], s, -1e30)
        m = jnp.max(s, axis=1, keepdims=True)
        p = jnp.exp(s - m)
        suf_top[j] = jnp.broadcast_to(m, (heads, 128))
        suf_tot[j] = jnp.broadcast_to(jnp.sum(p, axis=1, keepdims=True), (heads, 128))
        suf_out[j] = jnp.dot(p.astype(BF16), recent[:, :DL], preferred_element_type=F32)

    def parity_part():
        place = lax.broadcasted_iota(jnp.int32, (heads, 128), 0)
        for row in range(n_own):
            first = (row * n_slice + x) * per_dev
            odd = jnp.int32(0)
            for j in range(per_dev):
                slot = ps_ref[sp_ref[first + j]]
                odd = jnp.where((slot >> 1) == z, slot & 1, odd)
            parity[row * heads : (row + 1) * heads, :] = jnp.where(place >= 0, odd, 0)

    @pl.when(is_ring)
    def _():
        loads[0].wait()
        pl.semaphore_wait(barrier, 3)
        for k in range(len(pieces(0, 1))):
            for side in (0, 1):
                ring(side, 1, pieces(side, 1)[k]).start()
        loads[1].wait()
        raw().start()
        for load in loads[2:]:
            load.wait()
        filler = [functools.partial(recent_part, j) for j in range(per_dev)] + [parity_part]
        for k, (side, d, piece) in enumerate(every_piece()):
            ring(side, d, piece).wait_recv()
            if d < last and piece in pieces(side, d + 1):
                ring(side, d + 1, piece).start()
            pair(side, d, piece).start()
            if k % 2 == 1 and filler:
                filler.pop(0)()

    @pl.when(is_post)
    def _():
        for load in loads[:4]:
            load.wait()
        picks = own_places()

        def sample_of(row):
            pick = jnp.int32(0)
            for j in range(1, per_dev):
                pick = jnp.where(picks[j] == row, j, pick)
            return pick

        for row in range(n_own):
            stage[0, row] = q_vm[sample_of(row)]
        raw().wait_recv()
        for row in range(n_own):
            stage[1, row] = q_pair[sample_of(row)]
        arrived[z] = stage[0, z]
        pl.semaphore_wait(barrier, 2 * n_own - 1)
        for row in others():
            ask(0, row).start()
            ask(1, row).start()
        hand().start()
        loads[4].wait()
        loads[5].wait()
        parity_part()
        for j in range(per_dev):
            recent_part(j)
        for side, d, piece in every_piece():
            if d < last:
                pair(side, d, piece).wait_recv()

    def collect(lo, hi):
        for row in range(lo, hi):

            @pl.when(jnp.logical_or(is_ring, z != row))
            def _():
                asked_by(row).wait_recv()

    def weigh(lo, hi, begin, end):
        size = (hi - lo) * heads
        is_odd = parity[lo * heads : hi * heads, :1] > 0
        q = arrived[lo:hi].reshape(size, feat)
        s0 = jnp.dot(q, keys[0, :, begin:end], preferred_element_type=F32)
        s1 = jnp.dot(q, keys[1, :, begin:end], preferred_element_type=F32)
        s = jnp.where(is_odd, s1, s0) * scaling
        m = jnp.max(s, axis=1, keepdims=True)
        p = jnp.exp(s - m)
        l = jnp.sum(p, axis=1, keepdims=True)
        even = jnp.where(is_odd, 0.0, p).astype(BF16)
        odd = jnp.where(is_odd, p, 0.0).astype(BF16)
        out = lax.dot_general(
            even, keys[0, :DL, begin:end], NT, preferred_element_type=F32
        ) + lax.dot_general(odd, keys[1, :DL, begin:end], NT, preferred_element_type=F32)
        return m, l, out

    def give(lo, hi, m, l, out):
        size = (hi - lo) * heads
        lane = lax.broadcasted_iota(jnp.int32, (size, 128), 1)
        sub = lax.rem(lax.broadcasted_iota(jnp.int32, (size, 128), 0), heads)
        both = jnp.where(lane == sub, m, 0.0) + jnp.where(lane == sub + heads, l, 0.0)
        both = jnp.sum(both.reshape(hi - lo, heads, 128), axis=1)
        for row in range(lo, hi):
            at = row - lo
            stat[row] = both[at : at + 1, :]
            res[row] = out[at * heads : (at + 1) * heads, :].astype(BF16)
        for row in range(lo, hi):

            @pl.when(z != row)
            def _():
                answer(row).start()
                answer_stat(row).start()

    cut = n_own // SHARE
    near = (n_slice - 1) * tok
    collect(0, cut)
    m0, l0, out0 = weigh(0, cut, 0, near)
    part_top[...] = jnp.broadcast_to(m0, (cut * heads, 128))
    part_tot[...] = jnp.broadcast_to(l0, (cut * heads, 128))
    part_out[...] = out0

    @pl.when(is_post)
    def _():
        for side, d, piece in every_piece():
            if d == last:
                pair(side, d, piece).wait_recv()

    m1, l1, out1 = weigh(0, cut, near, near + tok)
    m0 = part_top[:, :1]
    m = jnp.maximum(m0, m1)
    fade0 = jnp.exp(m0 - m)
    fade1 = jnp.exp(m1 - m)
    give(0, cut, m, part_tot[:, :1] * fade0 + l1 * fade1, part_out[...] * fade0 + out1 * fade1)
    collect(cut, n_own)
    give(cut, n_own, *weigh(cut, n_own, 0, n_slice * tok))
    ret[z] = res[z]
    ret_stat[z] = stat[z]

    for row in others():
        answer(row).wait_send()
        answer_stat(row).wait_send()

    @pl.when(is_ring)
    def _():
        raw().wait_send()
        for side, d, piece in every_piece():
            ring(side, d, piece).wait_send()
            pair(side, d, piece).wait_send()

    @pl.when(is_post)
    def _():
        for row in others():
            ask(0, row).wait_send()
            ask(1, row).wait_send()
        hand().wait_send()

    places = own_places()
    for row in range(n_own):

        @pl.when(z != row)
        def _():
            for copy in answered_by(row):
                copy.wait_recv()

    lane8 = lax.broadcasted_iota(jnp.int32, (heads, 128), 1)
    sub8 = lax.broadcasted_iota(jnp.int32, (heads, 128), 0)
    for j in range(per_dev):
        line = jnp.broadcast_to(ret_stat[places[j]], (heads, 128))
        pre_top = jnp.sum(jnp.where(lane8 == sub8, line, 0.0), axis=1, keepdims=True)
        pre_tot = jnp.sum(jnp.where(lane8 == sub8 + heads, line, 0.0), axis=1, keepdims=True)
        own_top = suf_top[j][:, :1]
        own_tot = suf_tot[j][:, :1]
        m = jnp.maximum(pre_top, own_top)
        w_pre = jnp.exp(pre_top - m)
        w_own = jnp.exp(own_top - m)
        total = w_pre * pre_tot + w_own * own_tot
        num = w_pre * ret[places[j]].astype(F32) + w_own * suf_out[j]
        out_ref[j] = (num / total).astype(out_ref.dtype)


def solution(mesh):
    n_own = mesh.shape["prompt"]
    n_slice = mesh.shape["sample"]

    def body(queries, prompt_cache, suffix_cache, suffix_len, sample_prompt, prompt_slot):
        per_dev, heads, feat = queries.shape
        tok = prompt_cache.shape[1]
        ring = n_slice * P_DEV * PIECES
        dma = pltpu.SemaphoreType.DMA
        return pl.pallas_call(
            functools.partial(kernel, n_own, n_slice),
            out_shape=jax.ShapeDtypeStruct((per_dev, heads, DL), BF16),
            in_specs=[pl.BlockSpec(memory_space=pltpu.HBM)] * 6,
            out_specs=pl.BlockSpec(memory_space=pltpu.VMEM),
            scratch_shapes=[
                pltpu.SMEM(sample_prompt.shape, jnp.int32),
                pltpu.SMEM(prompt_slot.shape, jnp.int32),
                pltpu.SMEM(suffix_len.shape, jnp.int32),
                pltpu.VMEM(queries.shape, BF16),
                pltpu.VMEM(queries.shape, BF16),
                pltpu.VMEM((P_DEV, feat, n_slice * tok), BF16),
                pltpu.VMEM(suffix_cache.shape, BF16),
                pltpu.VMEM((2, n_own, heads, feat), BF16),
                pltpu.VMEM((n_own, heads, feat), BF16),
                pltpu.VMEM((n_own, heads, DL), BF16),
                pltpu.VMEM((n_own, 1, 128), F32),
                pltpu.VMEM((n_own, heads, DL), BF16),
                pltpu.VMEM((n_own, 1, 128), F32),
                pltpu.VMEM((per_dev, heads, DL), F32),
                pltpu.VMEM((per_dev, heads, 128), F32),
                pltpu.VMEM((per_dev, heads, 128), F32),
                pltpu.VMEM((n_own * heads, 128), jnp.int32),
                pltpu.VMEM((n_own // SHARE * heads, 128), F32),
                pltpu.VMEM((n_own // SHARE * heads, 128), F32),
                pltpu.VMEM((n_own // SHARE * heads, DL), F32),
                dma((6,)),
                dma((ring,)),
                dma((ring,)),
                dma((ring,)),
                dma((ring,)),
                dma((1,)),
                dma((1,)),
                dma((2, n_own)),
                dma((n_own,)),
                dma((n_own,)),
                dma((n_own,)),
                dma((n_own,)),
                dma((n_own,)),
            ],
            compiler_params=pltpu.CompilerParams(collective_id=0, has_side_effects=True),
        )(
            sample_prompt,
            prompt_slot,
            suffix_len,
            queries,
            jnp.swapaxes(prompt_cache, 1, 2),
            suffix_cache,
        )

    return jax.shard_map(
        body,
        mesh=mesh,
        in_specs=(
            P(("groups", "prompt", "sample"), "head", None),
            P(("groups", "prompt"), "sample", None),
            P(("groups", "prompt", "sample"), None, None),
            P(("groups", "prompt", "sample")),
            P("groups"),
            P("groups"),
        ),
        out_specs=P(("groups", "prompt", "sample"), "head", None),
        check_vma=False,
    )
```
